32 devices in a mesh: pp: 2 (over y), cp: 8 (over z, x), tp: 2 (over core).
Axes of the slice: x: 2, y: 2, z: 4, core: 2. Of those that a mesh axis runs over, the one named last changes fastest.
Arguments:
- queries: bfloat16 [2, 1024, 4096], P('pp', 'cp', 'tp'), may hold values from -4.5 to 4.5
- keys: bfloat16 [2, 1024, 256], P('pp', 'cp', 'tp'), may hold values from -4.5 to 4.5
- values: bfloat16 [2, 1024, 256], P('pp', 'cp', 'tp'), may hold values from -6 to 6
- out_weight: bfloat16 [4096, 16384], P('tp', 'cp'), may hold values from -1.5 to 1.5
- span_order: int32 [16], replicated, may hold values from 0 to 15, as said below
Outputs:
- handed: bfloat16 [2, 8, 128, 16384], P('pp', None, 'tp', 'cp')
The draws below stay inside these ranges and needn't reach their ends.
Inputs may be any that keep to these rules, and one draw needn't show every extreme that they name: `span_order`: the two stored blocks 2r and 2r + 1 are the sequence blocks j and 15 - j for some j, in either order; every sequence block appears once.
All inputs are finite; a program needn't handle non-finite values.
Results may differ from the reference program's by a relative error of at most 0.0095.
Values may be sent and summed in bfloat16 or wider, within the bound.
A program may use at most 128 MiB of HBM per device.

```python
import jax
import jax.numpy as jnp
from jax import lax

D = 16384
HEAD = 128
SPAN = 64
HEADS = 32
KVH = 2
TOKENS = 1024
N_PP = 2
N_CP = 8


def draw_keys(key, part):
    field = jnp.clip(jax.random.normal(jax.random.fold_in(key, 5), (N_PP, TOKENS, KVH * HEAD), jnp.float32), -4.5, 4.5)
    return field.astype(jnp.bfloat16)


def draw_queries(key, part):
    field = jnp.clip(jax.random.normal(jax.random.fold_in(key, 3), (N_PP, TOKENS, HEADS * HEAD), jnp.float32), -4.5, 4.5)
    return field.astype(jnp.bfloat16)


def draw_span_order(key, part):
    picked = jax.random.permutation(jax.random.fold_in(key, 21), N_CP)
    flipped = jax.random.randint(jax.random.fold_in(key, 22), (N_CP,), 0, 2)
    lower = jnp.where(flipped == 1, 2 * N_CP - 1 - picked, picked)
    upper = 2 * N_CP - 1 - lower
    return jnp.stack([lower, upper], axis=1).reshape(-1).astype(jnp.int32)


def block_levels(rng, extent, split, low, top_value):
    level = 1.0
    for axis_at, shards_of in split:
        draws = jax.random.uniform(jax.random.fold_in(jax.random.fold_in(rng, 6), axis_at), (shards_of,), jnp.float32, low / len(split), top_value / len(split))
        level = level * jnp.repeat(jnp.exp(draws), extent[axis_at] // shards_of).reshape((-1,) + (1,) * (len(extent) - 1 - axis_at))
    return level


def centred(stream_key, shape, deviation, reach, cuts=(), held_as=jnp.bfloat16):
    values = deviation * jax.random.normal(stream_key, shape, jnp.float32)
    if cuts:
        values = values * block_levels(stream_key, shape, cuts, -0.22, 0.18)
    return jnp.clip(values, -reach, reach).astype(held_as)


def setup_inputs(seed: int = 0) -> dict:
    key_of = jax.random.split(jax.random.key(seed), 6)
    return {
        "queries": draw_queries(jax.random.fold_in(key_of[5], 71), 0),
        "keys": draw_keys(jax.random.fold_in(key_of[5], 71), 0),
        "values": centred(key_of[2], (N_PP, TOKENS, KVH * HEAD), 1.0, 6.0, ((0, 2), (1, 8), (2, 2))),
        "out_weight": centred(key_of[3], (HEADS * HEAD, D), (max(HEADS * HEAD // 256, 1)) ** -0.5, 1.5, ((0, 2), (1, 8))),
        "span_order": draw_span_order(jax.random.fold_in(key_of[5], 71), 0),
    }


def reference(queries, keys, values, out_weight, span_order):
    offsets = jnp.arange(SPAN, dtype=jnp.int32)
    position = (span_order[:, None] * SPAN + offsets[None, :]).reshape(-1).astype(jnp.int32)
    allowed = position[None, :] <= position[:, None]
    group = HEADS // KVH
    scale = HEAD ** -0.5
    query_heads = queries.reshape(N_PP, TOKENS, HEADS, HEAD)
    key_heads = keys.reshape(N_PP, TOKENS, KVH, HEAD)
    value_heads = values.reshape(N_PP, TOKENS, KVH, HEAD)

    def single(index):
        section = index // HEADS
        head = index % HEADS
        query = query_heads[section, :, head]
        key_rows = key_heads[section, :, head // group]
        value_rows = value_heads[section, :, head // group]
        score = jnp.dot(query, key_rows.T, preferred_element_type=jnp.float32) * scale
        score = jnp.where(allowed, score, -1e30)
        summit = jnp.max(score, axis=-1, keepdims=True)
        weight = jnp.where(allowed, jnp.exp(score - summit), 0.0)
        total = jnp.sum(weight, axis=-1, keepdims=True)
        return jnp.dot(weight.astype(jnp.bfloat16), value_rows, preferred_element_type=jnp.float32) / total

    outputs = lax.map(single, jnp.arange(N_PP * HEADS, dtype=jnp.int32))
    attention = outputs.reshape(N_PP, HEADS, TOKENS, HEAD).transpose(0, 2, 1, 3)
    attention = attention.reshape(N_PP, TOKENS, HEADS * HEAD).astype(jnp.bfloat16)

    def project(section_rows):
        return jnp.dot(section_rows, out_weight, preferred_element_type=jnp.float32).astype(jnp.bfloat16)

    projected = lax.map(project, attention).reshape(N_PP, N_CP, 2 * SPAN, D)
    return jnp.roll(projected, 1, axis=0)
```

```python
import functools

import jax
import jax.numpy as jnp
from jax import lax
from jax.experimental import pallas as pl
from jax.experimental.pallas import tpu as pltpu
from jax.sharding import PartitionSpec as P

HEAD = 128
PARTS = 8
EXTRA = 4
FILL = 3
GIFT = 2
AHEAD = 3
OFF1 = 3
OFF2 = 7
OFF3 = 12
OFFG = 6
SIDE_END = 9
SIDE_MID = 9
LAG_END = 6
LAG_MID = 10
TILES = 4
NEAR = True
MESH = pl.DeviceIdType.MESH


def kernel(
    n_pp,
    n_cp,
    order_ref,
    q_ref,
    k_ref,
    v_ref,
    w_ref,
    out_ref,
    kv,
    qb,
    gs,
    ga,
    wb,
    acc,
    give,
    take,
    mask,
    in_sem,
    qin_sem,
    w_sem,
    kvs_sem,
    kvx_sem,
    kvr_sem,
    qs_sem,
    qg_sem,
    qr_sem,
    y_sem,
    up_sem,
    down_sem,
    x_sem,
    eu_sem,
    ed_sem,
    g_sem,
    ts_sem,
    tr_sem,
):
    pp, cp, tp = lax.axis_index("pp"), lax.axis_index("cp"), lax.axis_index("tp")
    line = n_cp // 2
    i, x = cp // 2, cp % 2
    side = i * 2 + 1 - x
    rows = kv.shape[2]
    half = rows // 2
    width = qb.shape[3]
    wide = wb.shape[1]
    tile = wide // TILES
    heads = width // HEAD
    after, before = lax.rem(pp + 1, n_pp), lax.rem(pp + n_pp - 1, n_pp)
    right = (pp, side, tp)
    sibling = (pp, cp, 1 - tp)
    has_up, has_down = i + 1 < line, i > 0
    end = (i == 0) | (i == line - 1)
    gift_down, gift_up = i == 1, i == line - 2
    giver = jnp.where(i == 0, 1, line - 2) * 2 + x

    def remote(src, dst, send, recv, device):
        return pltpu.make_async_remote_copy(
            src_ref=src,
            dst_ref=dst,
            send_sem=send,
            recv_sem=recv,
            device_id=device,
            device_id_type=MESH,
        )

    load_k = pltpu.make_async_copy(k_ref.at[0], kv.at[cp, 0], in_sem.at[0])
    load_v = pltpu.make_async_copy(v_ref.at[0], kv.at[cp, 1], in_sem.at[1])
    load_k.start()
    load_v.start()

    def load_q(s):
        at = pl.ds(pl.multiple_of(s * width, width), width)
        return pltpu.make_async_copy(q_ref.at[0, :, at], qb.at[0, s], qin_sem.at[s])

    @pl.loop(0, PARTS)
    def _(s):
        load_q(s).start()

    load_w = pltpu.make_async_copy(w_ref, wb, w_sem)
    load_w.start()

    barrier = pltpu.get_barrier_semaphore()

    def greet(device):
        pl.semaphore_signal(barrier, inc=1, device_id=device, device_id_type=MESH)

    @pl.loop(0, line)
    def _(j):
        @pl.when(j != i)
        def _():
            greet((pp, j * 2 + x, tp))

    greet((after, cp, tp))
    greet((before, cp, tp))
    greet(right)
    greet(sibling)
    load_k.wait()
    load_v.wait()
    pl.semaphore_wait(barrier, line + 3)

    def kv_line(j):
        return remote(kv.at[cp], kv.at[cp], kvs_sem.at[j], kvr_sem.at[cp], (pp, j * 2 + x, tp))

    def kv_pass(c):
        return remote(kv.at[c], kv.at[c], kvx_sem.at[c // 2], kvr_sem.at[c], right)

    def q_side(s):
        return remote(qb.at[0, s], qb.at[1, s], qs_sem, qr_sem.at[0, s], right)

    def q_gift(s, to):
        return remote(qb.at[0, s], qb.at[2, s], qg_sem.at[to], qr_sem.at[1, s], (pp, cp - 2 + 4 * to, tp))

    def in_turn(body):
        @pl.loop(0, line - 1)
        def _(e):
            d = e + 1 if NEAR else line - 1 - e
            for j, inside in ((i - d, i - d >= 0), (i + d, i + d < line)):

                @pl.when(inside)
                def _():
                    body(j)

    in_turn(lambda j: kv_line(j).start())
    kv_pass(cp).start()

    @pl.loop(0, PARTS)
    def _(s):
        load_q(s).wait()

        @pl.when(s < FILL)
        def _():
            q_side(s).start()

        for to, there in ((0, gift_down), (1, gift_up)):

            @pl.when(there & (s >= PARTS - GIFT))
            def _():
                q_gift(s, to).start()

    row = lax.broadcasted_iota(jnp.int32, (rows, 1), 0)
    col = lax.broadcasted_iota(jnp.int32, (1, rows), 1)
    for which, block in ((0, cp), (1, side), (2, giver)):
        query_pos = row + jnp.where(row < half, order_ref[2 * block] * half, order_ref[2 * block + 1] * half - half)
        for c in range(n_cp):
            key_pos = col + jnp.where(col < half, order_ref[2 * c] * half, order_ref[2 * c + 1] * half - half)
            mask[which, :, c * rows : (c + 1) * rows] = jnp.where(key_pos <= query_pos, 0.0, -1e30)

    def pass_kv(j):
        kv_pass(j * 2 + x).wait_recv()
        kv_pass(j * 2 + x).start()

    in_turn(pass_kv)

    @pl.loop(FILL, PARTS)
    def _(s):
        q_side(s).start()

    @pl.loop(0, line)
    def _(j):
        kv_pass(j * 2 + 1 - x).wait_recv()

    factor = HEAD ** (-0.5) * 1.4426950408889634
    length = n_cp * rows

    def send_after(which, c, s):
        return remote(gs.at[which, s], ga.at[c, s], y_sem.at[which], g_sem.at[c, s], (after, cp, tp))

    gifts = jnp.where(end, GIFT, 0)

    def attend(a):
        own, gift = a < PARTS, a < PARTS + gifts
        which = jnp.where(own, 0, jnp.where(gift, 2, 1))
        s = a - jnp.where(own, 0, jnp.where(gift, GIFT, PARTS + gifts))

        @pl.when(which == 1)
        def _():
            q_side(s).wait_recv()

        @pl.when(which == 2)
        def _():
            q_gift(s, 0).wait_recv()

        keys = kv[:, 0].reshape(length, HEAD)
        values = kv[:, 1].reshape(length, HEAD)
        for h in range(heads):
            at = slice(h * HEAD, (h + 1) * HEAD)
            score = lax.dot_general(
                qb[which, s, :, at], keys, (((1,), (1,)), ((), ())), preferred_element_type=jnp.float32
            )
            score = score + mask[which]
            weight = jnp.exp2((score - jnp.max(score, axis=1, keepdims=True)) * factor)
            total = jnp.sum(weight, axis=1, keepdims=True)
            mixed = jnp.dot(weight.astype(jnp.bfloat16), values, preferred_element_type=jnp.float32)
            gs[which, s, :, at] = (mixed / total).astype(jnp.bfloat16)
        send_after(which, jnp.where(own, cp, jnp.where(gift, giver, side)), s).start()

    def send_up(c, s):
        return remote(ga.at[c, s], ga.at[c, s], up_sem.at[c // 2], g_sem.at[c, s], (pp, cp + 2, tp))

    def send_down(c, s):
        return remote(ga.at[c, s], ga.at[c, s], down_sem.at[c // 2], g_sem.at[c, s], (pp, cp - 2, tp))

    def send_side(c, s):
        return remote(ga.at[c, s], ga.at[c, s], x_sem.at[c // 2], g_sem.at[c, s], right)

    def extra_up(s):
        return remote(ga.at[side, s], ga.at[side, s], eu_sem, g_sem.at[side, s], (pp, cp + 2, tp))

    def extra_down(s):
        return remote(ga.at[side, s], ga.at[side, s], ed_sem, g_sem.at[side, s], (pp, cp - 2, tp))

    def swap(c):
        return remote(give.at[c], take.at[c], ts_sem.at[c], tr_sem.at[c], sibling)

    def arrived(c, s):
        send_side(c, s).wait_recv()

    def project(c, p):
        for n in range(TILES):
            cols = slice(n * tile, (n + 1) * tile)
            term = None
            for r in range(2):
                at = pl.ds(pl.multiple_of((2 * p + r) * width, width), width)
                piece = jnp.dot(ga[c, 2 * p + r], wb[at, cols], preferred_element_type=jnp.float32)
                term = piece if term is None else term + piece
            acc[c, :, cols] = jnp.where(p == 0, 0.0, acc[c, :, cols]) + term

    def settle(c):
        theirs = pl.ds(pl.multiple_of((1 - tp) * half, half), half)
        give[c] = acc[c, theirs, :].astype(jnp.bfloat16)
        swap(c).start()

    def finish(c):
        ours = pl.ds(pl.multiple_of(tp * half, half), half)
        swap(c).wait_recv()
        out_ref[0, c] = (acc[c, ours, :] + take[c].astype(jnp.float32)).astype(jnp.bfloat16)

    def consume(c, s):
        @pl.when(s % 2 == 1)
        def _():
            project(c, s // 2)

            @pl.when(s == PARTS - 1)
            def _():
                settle(c)

    @pl.loop(0, AHEAD)
    def _(a):
        attend(a)

    load_w.wait()
    lag = jnp.where(end, LAG_END, LAG_MID)
    side_at = jnp.where(end, SIDE_END, SIDE_MID)
    given = PARTS - GIFT

    def passed(d):
        return jnp.where(d == 0, 0, jnp.where(d == 1, OFF1, jnp.where(d == 2, OFF2, OFF3 + (d - 3) * PARTS))) + PARTS

    last_up = jnp.maximum(passed(i), side_at + PARTS) - 1
    last_down = jnp.maximum(passed(line - 1 - i), side_at + PARTS) - 1
    ticks = max(max(OFF2, OFF3 + (line - 4) * PARTS) + max(LAG_END, LAG_MID), SIDE_END, SIDE_MID) + PARTS

    def by_side(d, s):
        return (d > 1) | (s < PARTS - EXTRA)

    def slot(k, tick):
        early = tick < OFF3 + (k % 2) * PARTS
        since = tick - OFF3 - (k % 2) * PARTS
        d = jnp.where(early, 1 + k % 2, 3 + k % 2 + 2 * (since // (2 * PARTS)))
        s = jnp.where(early, tick - jnp.where(k == 0, OFF1, OFF2), lax.rem(since + 2 * PARTS, 2 * PARTS))
        d, s = jnp.where(k == 2, 1, d), jnp.where(k == 2, tick - OFFG, s)
        gift = end & (d == 1) & (s >= given)
        return d, s, (s >= 0) & (s < PARTS) & (d < line) & (gift == (k == 2))

    def places(tick, body):
        @pl.loop(0, 3)
        def _(k):
            d, s, there = slot(k, tick)

            @pl.when(there)
            def _():
                body(d, s)

    @pl.loop(0, ticks)
    def _(tick):
        @pl.when(tick < PARTS)
        def _():
            arrived(cp, tick)

            @pl.when(has_up & ~(gift_up & (tick >= given)))
            def _():
                send_up(cp, tick).start()

            @pl.when(has_down & ~(gift_down & (tick >= given)))
            def _():
                send_down(cp, tick).start()

        def relay(d, s):
            @pl.when(i - d >= 0)
            def _():
                c = cp - 2 * d
                arrived(c, s)

                @pl.when(has_up)
                def _():
                    send_up(c, s).start()

                @pl.when(by_side(d, s))
                def _():
                    send_side(c, s).start()

            @pl.when(i + d < line)
            def _():
                c = cp + 2 * d
                arrived(c, s)

                @pl.when(has_down)
                def _():
                    send_down(c, s).start()

                @pl.when(by_side(d, s))
                def _():
                    send_side(c, s).start()

        places(tick, relay)

        @pl.when(tick + AHEAD < 2 * PARTS + gifts)
        def _():
            attend(tick + AHEAD)

        @pl.when(tick < PARTS)
        def _():
            consume(cp, tick)

        @pl.when((tick >= side_at) & (tick < side_at + PARTS))
        def _():
            arrived(side, tick - side_at)
            consume(side, tick - side_at)

        @pl.when(has_up & (tick == last_up))
        def _():
            @pl.loop(PARTS - EXTRA, PARTS)
            def _(r):
                extra_up(r).start()

        @pl.when(has_down & (tick == last_down))
        def _():
            @pl.loop(PARTS - EXTRA, PARTS)
            def _(r):
                extra_down(r).start()

        def absorb(d, s):
            @pl.loop(0, 2)
            def _(far):
                j = i + (2 * far - 1) * d

                @pl.when((j >= 0) & (j < line))
                def _():
                    consume(j * 2 + x, s)

        places(tick, absorb)

        @pl.when(tick == PARTS + 4)
        def _():
            finish(cp)

        @pl.when(tick == side_at + PARTS - 1)
        def _():
            finish(side)

        for d, at in ((1, max(OFF1, OFFG)), (2, OFF2)):
            if d < line:

                @pl.when(tick == at + PARTS + 3)
                def _():
                    @pl.when(i - d >= 0)
                    def _():
                        finish(cp - 2 * d)

                    @pl.when(i + d < line)
                    def _():
                        finish(cp + 2 * d)

        def absorb_side(d, s):
            @pl.loop(0, 2)
            def _(far):
                j = i + (2 * far - 1) * d

                @pl.when((j >= 0) & (j < line) & by_side(d, s))
                def _():
                    arrived(j * 2 + 1 - x, s)
                    consume(j * 2 + 1 - x, s)

        places(tick - lag, absorb_side)

    @pl.loop(3, line)
    def _(d):
        @pl.when(i - d >= 0)
        def _():
            finish(cp - 2 * d)

        @pl.when(i + d < line)
        def _():
            finish(cp + 2 * d)

    @pl.loop(PARTS - EXTRA, PARTS)
    def _(r):
        @pl.loop(0, 2)
        def _(far):
            j = i + 2 * far - 1

            @pl.when((j >= 0) & (j < line))
            def _():
                arrived(j * 2 + 1 - x, r)
                consume(j * 2 + 1 - x, r)

    @pl.loop(1, line)
    def _(e):
        d = line - e

        @pl.when(i - d >= 0)
        def _():
            finish(side - 2 * d)

        @pl.when(i + d < line)
        def _():
            finish(side + 2 * d)

    in_turn(lambda j: kv_line(j).wait_send())

    def left(ref, sem):
        remote(ref, ref, sem, g_sem.at[0, 0], right).wait_send()

    @pl.loop(0, line)
    def _(j):
        c = j * 2 + x
        kv_pass(c).wait_send()
        near = jnp.abs(j - i) == 1

        @pl.when((j != i) & ~near)
        def _():
            left(ga.at[c], x_sem.at[j])

        @pl.when(near)
        def _():
            left(ga.at[c, 0 : PARTS - EXTRA], x_sem.at[j])

        for there, sem, short in (
            ((j <= i) & has_up, up_sem, gift_up & (j == i)),
            ((j >= i) & has_down, down_sem, gift_down & (j == i)),
        ):

            @pl.when(there & short)
            def _():
                left(ga.at[c, 0:given], sem.at[j])

            @pl.when(there & ~short)
            def _():
                left(ga.at[c], sem.at[j])

    left(qb.at[0], qs_sem)
    left(gs.at[0], y_sem.at[0])
    left(gs.at[1], y_sem.at[1])

    @pl.when(end)
    def _():
        left(gs.at[2, given:PARTS], y_sem.at[2])

    for to, there in ((0, gift_down), (1, gift_up)):

        @pl.when(there)
        def _():
            left(qb.at[0, given:PARTS], qg_sem.at[to])

    @pl.when(has_up)
    def _():
        left(ga.at[side, PARTS - EXTRA : PARTS], eu_sem)

    @pl.when(has_down)
    def _():
        left(ga.at[side, PARTS - EXTRA : PARTS], ed_sem)

    @pl.loop(0, n_cp)
    def _(c):
        swap(c).wait_send()


def on_device(n_pp, n_cp, queries, keys, values, out_weight, span_order):
    rows = queries.shape[1]
    half = rows // 2
    depth, wide = out_weight.shape
    width = depth // PARTS
    line = n_cp // 2
    hbm = pl.BlockSpec(memory_space=pl.ANY)
    dma = pltpu.SemaphoreType.DMA
    queries, keys, values, out_weight, span_order = (
        pltpu.with_memory_space_constraint(a, pltpu.HBM)
        for a in (queries, keys, values, out_weight, span_order)
    )
    return pl.pallas_call(
        functools.partial(kernel, n_pp, n_cp),
        out_shape=pltpu.VMEM((1, n_cp, half, wide), jnp.bfloat16),
        in_specs=[pl.BlockSpec(memory_space=pltpu.SMEM), hbm, hbm, hbm, hbm],
        out_specs=pl.BlockSpec(memory_space=pltpu.VMEM),
        scratch_shapes=[
            pltpu.VMEM((n_cp, 2, rows, HEAD), jnp.bfloat16),
            pltpu.VMEM((3, PARTS, rows, width), jnp.bfloat16),
            pltpu.VMEM((3, PARTS, rows, width), jnp.bfloat16),
            pltpu.VMEM((n_cp, PARTS, rows, width), jnp.bfloat16),
            pltpu.VMEM((depth, wide), jnp.bfloat16),
            pltpu.VMEM((n_cp, rows, wide), jnp.float32),
            pltpu.VMEM((n_cp, half, wide), jnp.bfloat16),
            pltpu.VMEM((n_cp, half, wide), jnp.bfloat16),
            pltpu.VMEM((3, rows, n_cp * rows), jnp.float32),
            dma((2,)),
            dma((PARTS,)),
            dma,
            dma((line,)),
            dma((line,)),
            dma((n_cp,)),
            dma,
            dma((2,)),
            dma((2, PARTS)),
            dma((3,)),
            dma((line,)),
            dma((line,)),
            dma((line,)),
            dma,
            dma,
            dma((n_cp, PARTS)),
            dma((n_cp,)),
            dma((n_cp,)),
        ],
        compiler_params=pltpu.CompilerParams(
            collective_id=0, has_side_effects=True, vmem_limit_bytes=50000 * 1024
        ),
    )(span_order, queries, keys, values, out_weight)


def solution(mesh):
    placed = (P("pp", "cp", "tp"), P("pp", "cp", "tp"), P("pp", "cp", "tp"), P("tp", "cp"), P())
    return jax.shard_map(
        functools.partial(on_device, mesh.shape["pp"], mesh.shape["cp"]),
        mesh=mesh,
        in_specs=placed,
        out_specs=P("pp", None, "tp", "cp"),
        check_vma=False,
    )
```

```python
import functools

import jax
import jax.numpy as jnp
from jax import lax
from jax.experimental import pallas as pl
from jax.experimental.pallas import tpu as pltpu
from jax.sharding import PartitionSpec as P

HEAD = 128
PARTS = 8
EXTRA = 4
FILL = 3
GIFT = 4
AHEAD = 5
OFF1 = 3
OFF2 = 7
OFF3 = 13
OFFG = 6
SIDE_END = 11
SIDE_MID = 10
LAG_END = 7
LAG_MID = 6
TILES = 4
NEAR = True
SPAN = 256
GROUP = 4
MESH = pl.DeviceIdType.MESH


def kernel(
    n_pp,
    n_cp,
    order_ref,
    q_ref,
    k_ref,
    v_ref,
    w_ref,
    out_ref,
    kv,
    qb,
    gs,
    ga,
    wb,
    acc,
    give,
    take,
    mask,
    in_sem,
    qin_sem,
    w_sem,
    kvs_sem,
    kvx_sem,
    kvr_sem,
    qs_sem,
    qg_sem,
    qr_sem,
    y_sem,
    up_sem,
    down_sem,
    x_sem,
    eu_sem,
    ed_sem,
    g_sem,
    ts_sem,
    tr_sem,
):
    pp, cp, tp = lax.axis_index("pp"), lax.axis_index("cp"), lax.axis_index("tp")
    line = n_cp // 2
    i, x = cp // 2, cp % 2
    side = i * 2 + 1 - x
    rows = kv.shape[2]
    half = rows // 2
    width = qb.shape[3]
    wide = wb.shape[1]
    tile = wide // TILES
    heads = width // HEAD
    after, before = lax.rem(pp + 1, n_pp), lax.rem(pp + n_pp - 1, n_pp)
    right = (pp, side, tp)
    sibling = (pp, cp, 1 - tp)
    has_up, has_down = i + 1 < line, i > 0
    end = (i == 0) | (i == line - 1)
    gift_down, gift_up = i == 1, i == line - 2
    giver = jnp.where(i == 0, 1, line - 2) * 2 + x

    def remote(src, dst, send, recv, device):
        return pltpu.make_async_remote_copy(
            src_ref=src,
            dst_ref=dst,
            send_sem=send,
            recv_sem=recv,
            device_id=device,
            device_id_type=MESH,
        )

    load_k = pltpu.make_async_copy(k_ref.at[0], kv.at[cp, 0], in_sem.at[0])
    load_v = pltpu.make_async_copy(v_ref.at[0], kv.at[cp, 1], in_sem.at[1])
    load_k.start()
    load_v.start()

    def load_q(s):
        at = pl.ds(pl.multiple_of(s * width, width), width)
        return pltpu.make_async_copy(q_ref.at[0, :, at], qb.at[0, s], qin_sem.at[s])

    @pl.loop(0, PARTS)
    def _(s):
        load_q(s).start()

    load_w = pltpu.make_async_copy(w_ref, wb, w_sem)
    load_w.start()

    barrier = pltpu.get_barrier_semaphore()

    def greet(device):
        pl.semaphore_signal(barrier, inc=1, device_id=device, device_id_type=MESH)

    @pl.loop(0, line)
    def _(j):
        @pl.when(j != i)
        def _():
            greet((pp, j * 2 + x, tp))

    greet((after, cp, tp))
    greet((before, cp, tp))
    greet(right)
    greet(sibling)
    load_k.wait()
    load_v.wait()
    pl.semaphore_wait(barrier, line + 3)

    def kv_line(j):
        return remote(kv.at[cp], kv.at[cp], kvs_sem.at[j], kvr_sem.at[cp], (pp, j * 2 + x, tp))

    def kv_pass(c):
        return remote(kv.at[c], kv.at[c], kvx_sem.at[c // 2], kvr_sem.at[c], right)

    def q_side(s):
        return remote(qb.at[0, s], qb.at[1, s], qs_sem, qr_sem.at[0, s], right)

    def q_gift(s, to):
        return remote(qb.at[0, s], qb.at[2, s], qg_sem.at[to], qr_sem.at[1, s], (pp, cp - 2 + 4 * to, tp))

    def in_turn(body):
        @pl.loop(0, line - 1)
        def _(e):
            d = e + 1 if NEAR else line - 1 - e
            for j, inside in ((i - d, i - d >= 0), (i + d, i + d < line)):

                @pl.when(inside)
                def _():
                    body(j)

    in_turn(lambda j: kv_line(j).start())
    kv_pass(cp).start()

    @pl.loop(0, PARTS)
    def _(s):
        load_q(s).wait()

        @pl.when(s < FILL)
        def _():
            q_side(s).start()

        for to, there in ((0, gift_down), (1, gift_up)):

            @pl.when(there & (s >= PARTS - GIFT))
            def _():
                q_gift(s, to).start()

    row = lax.broadcasted_iota(jnp.int32, (rows, 1), 0)
    col = lax.broadcasted_iota(jnp.int32, (1, rows), 1)
    for which, block in ((0, cp), (1, side), (2, giver)):
        query_pos = row + jnp.where(row < half, order_ref[2 * block] * half, order_ref[2 * block + 1] * half - half)
        for c in range(n_cp):
            key_pos = col + jnp.where(col < half, order_ref[2 * c] * half, order_ref[2 * c + 1] * half - half)
            mask[which, :, c * rows : (c + 1) * rows] = jnp.where(key_pos <= query_pos, 0.0, -1e30)

    def pass_kv(j):
        kv_pass(j * 2 + x).wait_recv()
        kv_pass(j * 2 + x).start()

    in_turn(pass_kv)

    @pl.loop(FILL, PARTS)
    def _(s):
        q_side(s).start()

    @pl.loop(0, line)
    def _(j):
        kv_pass(j * 2 + 1 - x).wait_recv()

    factor = HEAD ** (-0.5) * 1.4426950408889634
    length = n_cp * rows

    def send_after(which, c, s):
        return remote(gs.at[which, s], ga.at[c, s], y_sem.at[which], g_sem.at[c, s], (after, cp, tp))

    gifts = jnp.where(end, GIFT, 0)

    def attend(a):
        own, gift = a < PARTS, a < PARTS + gifts
        which = jnp.where(own, 0, jnp.where(gift, 2, 1))
        s = a - jnp.where(own, 0, jnp.where(gift, GIFT, PARTS + gifts))

        @pl.when(which == 1)
        def _():
            q_side(s).wait_recv()

        @pl.when(which == 2)
        def _():
            q_gift(s, 0).wait_recv()

        blocks = SPAN // rows
        spans = [(slice(b * blocks, (b + 1) * blocks), slice(b * SPAN, (b + 1) * SPAN)) for b in range(length // SPAN)]

        def scores(h):
            query = qb[which, s, :, h * HEAD : (h + 1) * HEAD]
            return [
                lax.dot_general(
                    query,
                    kv[b, 0].reshape(SPAN, HEAD),
                    (((1,), (1,)), ((), ())),
                    preferred_element_type=jnp.float32,
                )
                + mask[which, :, at]
                for b, at in spans
            ]

        ready = scores(0)
        for h in range(heads):
            score = ready
            if h + 1 < heads:
                ready = scores(h + 1)
            top = jnp.max(functools.reduce(jnp.maximum, score), axis=1, keepdims=True)
            weight = [jnp.exp2((z - top) * factor) for z in score]
            total = jnp.sum(functools.reduce(jnp.add, weight), axis=1, keepdims=True)
            mixed = None
            for (b, _), w in zip(spans, weight):
                term = jnp.dot(
                    w.astype(jnp.bfloat16), kv[b, 1].reshape(SPAN, HEAD), preferred_element_type=jnp.float32
                )
                mixed = term if mixed is None else mixed + term
            gs[which, s, :, h * HEAD : (h + 1) * HEAD] = (mixed / total).astype(jnp.bfloat16)
        send_after(which, jnp.where(own, cp, jnp.where(gift, giver, side)), s).start()

    def send_up(c, s):
        return remote(ga.at[c, s], ga.at[c, s], up_sem.at[c // 2], g_sem.at[c, s], (pp, cp + 2, tp))

    def send_down(c, s):
        return remote(ga.at[c, s], ga.at[c, s], down_sem.at[c // 2], g_sem.at[c, s], (pp, cp - 2, tp))

    def send_side(c, s):
        return remote(ga.at[c, s], ga.at[c, s], x_sem.at[c // 2], g_sem.at[c, s], right)

    def extra_up(s):
        return remote(ga.at[side, s], ga.at[side, s], eu_sem, g_sem.at[side, s], (pp, cp + 2, tp))

    def extra_down(s):
        return remote(ga.at[side, s], ga.at[side, s], ed_sem, g_sem.at[side, s], (pp, cp - 2, tp))

    def swap(c):
        return remote(give.at[c], take.at[c], ts_sem.at[c], tr_sem.at[c], sibling)

    def arrived(c, s):
        send_side(c, s).wait_recv()

    def project(c, p):
        for n in range(TILES):
            cols = slice(n * tile, (n + 1) * tile)
            term = None
            for r in range(GROUP):
                at = pl.ds(pl.multiple_of((GROUP * p + r) * width, width), width)
                piece = jnp.dot(ga[c, GROUP * p + r], wb[at, cols], preferred_element_type=jnp.float32)
                term = piece if term is None else term + piece
            acc[c, :, cols] = jnp.where(p == 0, 0.0, acc[c, :, cols]) + term

    def settle(c):
        theirs = pl.ds(pl.multiple_of((1 - tp) * half, half), half)
        give[c] = acc[c, theirs, :].astype(jnp.bfloat16)
        swap(c).start()

    def finish(c):
        ours = pl.ds(pl.multiple_of(tp * half, half), half)
        swap(c).wait_recv()
        out_ref[0, c] = (acc[c, ours, :] + take[c].astype(jnp.float32)).astype(jnp.bfloat16)

    def consume(c, s):
        project(c, s // GROUP)

        @pl.when(s == PARTS - 1)
        def _():
            settle(c)

    def complete(s):
        return s % GROUP == GROUP - 1

    @pl.loop(0, AHEAD)
    def _(a):
        attend(a)

    load_w.wait()
    lag = jnp.where(end, LAG_END, LAG_MID)
    side_at = jnp.where(end, SIDE_END, SIDE_MID)
    given = PARTS - GIFT

    def passed(d):
        return jnp.where(d == 0, 0, jnp.where(d == 1, OFF1, jnp.where(d == 2, OFF2, OFF3 + (d - 3) * PARTS))) + PARTS

    last_up = jnp.maximum(passed(i), side_at + PARTS) - 1
    last_down = jnp.maximum(passed(line - 1 - i), side_at + PARTS) - 1
    ticks = max(max(OFF2, OFF3 + (line - 4) * PARTS) + max(LAG_END, LAG_MID), SIDE_END + 3, SIDE_MID + 3) + PARTS

    def by_side(d, s):
        return (d > 1) | (s < PARTS - EXTRA)

    def slot(k, tick):
        early = tick < OFF3 + (k % 2) * PARTS
        since = tick - OFF3 - (k % 2) * PARTS
        d = jnp.where(early, 1 + k % 2, 3 + k % 2 + 2 * (since // (2 * PARTS)))
        s = jnp.where(early, tick - jnp.where(k == 0, OFF1, OFF2), lax.rem(since + 2 * PARTS, 2 * PARTS))
        d, s = jnp.where(k == 2, 1, d), jnp.where(k == 2, tick - OFFG, s)
        gift = end & (d == 1) & (s >= given)
        return d, s, (s >= 0) & (s < PARTS) & (d < line) & (gift == (k == 2))

    @pl.loop(0, ticks)
    def _(tick):
        @pl.when(tick < PARTS)
        def _():
            arrived(cp, tick)

            @pl.when(has_up & ~(gift_up & (tick >= given)))
            def _():
                send_up(cp, tick).start()

            @pl.when(has_down & ~(gift_down & (tick >= given)))
            def _():
                send_down(cp, tick).start()

        def relay(d, s):
            @pl.when(i - d >= 0)
            def _():
                c = cp - 2 * d
                arrived(c, s)

                @pl.when(has_up)
                def _():
                    send_up(c, s).start()

                @pl.when(by_side(d, s))
                def _():
                    send_side(c, s).start()

            @pl.when(i + d < line)
            def _():
                c = cp + 2 * d
                arrived(c, s)

                @pl.when(has_down)
                def _():
                    send_down(c, s).start()

                @pl.when(by_side(d, s))
                def _():
                    send_side(c, s).start()

        for k in range(3):
            d, s, there = slot(k, tick)

            @pl.when(there)
            def _():
                relay(d, s)

        @pl.when(tick + AHEAD < 2 * PARTS + gifts)
        def _():
            attend(tick + AHEAD)

        beside = tick - side_at

        @pl.when((beside >= 0) & (beside < PARTS))
        def _():
            arrived(side, beside)

        @pl.when(has_up & (tick == last_up))
        def _():
            @pl.loop(PARTS - EXTRA, PARTS)
            def _(r):
                extra_up(r).start()

        @pl.when(has_down & (tick == last_down))
        def _():
            @pl.loop(PARTS - EXTRA, PARTS)
            def _(r):
                extra_down(r).start()

        @pl.when(tick == PARTS + 4)
        def _():
            finish(cp)

        @pl.when(tick == side_at + PARTS + 2)
        def _():
            finish(side)

        for d, at in ((1, max(OFF1, OFFG)), (2, OFF2)):
            if d < line:

                @pl.when(tick == at + PARTS + 3)
                def _():
                    @pl.when(i - d >= 0)
                    def _():
                        finish(cp - 2 * d)

                    @pl.when(i + d < line)
                    def _():
                        finish(cp + 2 * d)

        @pl.loop(0, 8)
        def _(k):
            over = k // 4
            place = k % 4
            d, s, there = slot(place, tick - over * lag)
            home = jnp.where(over == 1, beside, tick)
            d, s = jnp.where(place == 3, 0, d), jnp.where(place == 3, home, s)
            there = jnp.where(place == 3, ((home >= 0) & (home < PARTS)).astype(jnp.int32), there.astype(jnp.int32))
            column = jnp.where(over == 1, 1 - x, x)
            apart = (over == 1) & (d > 0)

            @pl.when((there == 1) & complete(s) & (~apart | by_side(d, s)))
            def _():
                @pl.loop(jnp.where(d == 0, 1, 0), 2)
                def _(far):
                    j = i + (2 * far - 1) * d
                    c = j * 2 + column

                    @pl.when((j >= 0) & (j < line))
                    def _():
                        @pl.when(apart)
                        def _():
                            @pl.loop(0, GROUP)
                            def _(r):
                                arrived(c, s - (GROUP - 1) + r)

                        consume(c, s)

    @pl.loop(3, line)
    def _(d):
        @pl.when(i - d >= 0)
        def _():
            finish(cp - 2 * d)

        @pl.when(i + d < line)
        def _():
            finish(cp + 2 * d)

    @pl.loop(PARTS - EXTRA, PARTS)
    def _(r):
        @pl.loop(0, 2)
        def _(far):
            j = i + 2 * far - 1

            @pl.when((j >= 0) & (j < line))
            def _():
                arrived(j * 2 + 1 - x, r)

                @pl.when(complete(r))
                def _():
                    consume(j * 2 + 1 - x, r)

    @pl.loop(1, line)
    def _(e):
        d = line - e

        @pl.when(i - d >= 0)
        def _():
            finish(side - 2 * d)

        @pl.when(i + d < line)
        def _():
            finish(side + 2 * d)

    in_turn(lambda j: kv_line(j).wait_send())

    def left(ref, sem):
        remote(ref, ref, sem, g_sem.at[0, 0], right).wait_send()

    @pl.loop(0, line)
    def _(j):
        c = j * 2 + x
        kv_pass(c).wait_send()
        near = jnp.abs(j - i) == 1

        @pl.when((j != i) & ~near)
        def _():
            left(ga.at[c], x_sem.at[j])

        @pl.when(near)
        def _():
            left(ga.at[c, 0 : PARTS - EXTRA], x_sem.at[j])

        for there, sem, short in (
            ((j <= i) & has_up, up_sem, gift_up & (j == i)),
            ((j >= i) & has_down, down_sem, gift_down & (j == i)),
        ):

            @pl.when(there & short)
            def _():
                left(ga.at[c, 0:given], sem.at[j])

            @pl.when(there & ~short)
            def _():
                left(ga.at[c], sem.at[j])

    left(qb.at[0], qs_sem)
    left(gs.at[0], y_sem.at[0])
    left(gs.at[1], y_sem.at[1])

    @pl.when(end)
    def _():
        left(gs.at[2, given:PARTS], y_sem.at[2])

    for to, there in ((0, gift_down), (1, gift_up)):

        @pl.when(there)
        def _():
            left(qb.at[0, given:PARTS], qg_sem.at[to])

    @pl.when(has_up)
    def _():
        left(ga.at[side, PARTS - EXTRA : PARTS], eu_sem)

    @pl.when(has_down)
    def _():
        left(ga.at[side, PARTS - EXTRA : PARTS], ed_sem)

    @pl.loop(0, n_cp)
    def _(c):
        swap(c).wait_send()


def on_device(n_pp, n_cp, queries, keys, values, out_weight, span_order):
    rows = queries.shape[1]
    half = rows // 2
    depth, wide = out_weight.shape
    width = depth // PARTS
    line = n_cp // 2
    hbm = pl.BlockSpec(memory_space=pl.ANY)
    dma = pltpu.SemaphoreType.DMA
    queries, keys, values, out_weight, span_order = (
        pltpu.with_memory_space_constraint(a, pltpu.HBM)
        for a in (queries, keys, values, out_weight, span_order)
    )
    return pl.pallas_call(
        functools.partial(kernel, n_pp, n_cp),
        out_shape=pltpu.VMEM((1, n_cp, half, wide), jnp.bfloat16),
        in_specs=[pl.BlockSpec(memory_space=pltpu.SMEM), hbm, hbm, hbm, hbm],
        out_specs=pl.BlockSpec(memory_space=pltpu.VMEM),
        scratch_shapes=[
            pltpu.VMEM((n_cp, 2, rows, HEAD), jnp.bfloat16),
            pltpu.VMEM((3, PARTS, rows, width), jnp.bfloat16),
            pltpu.VMEM((3, PARTS, rows, width), jnp.bfloat16),
            pltpu.VMEM((n_cp, PARTS, rows, width), jnp.bfloat16),
            pltpu.VMEM((depth, wide), jnp.bfloat16),
            pltpu.VMEM((n_cp, rows, wide), jnp.float32),
            pltpu.VMEM((n_cp, half, wide), jnp.bfloat16),
            pltpu.VMEM((n_cp, half, wide), jnp.bfloat16),
            pltpu.VMEM((3, rows, n_cp * rows), jnp.float32),
            dma((2,)),
            dma((PARTS,)),
            dma,
            dma((line,)),
            dma((line,)),
            dma((n_cp,)),
            dma,
            dma((2,)),
            dma((2, PARTS)),
            dma((3,)),
            dma((line,)),
            dma((line,)),
            dma((line,)),
            dma,
            dma,
            dma((n_cp, PARTS)),
            dma((n_cp,)),
            dma((n_cp,)),
        ],
        compiler_params=pltpu.CompilerParams(
            collective_id=0, has_side_effects=True, vmem_limit_bytes=50000 * 1024
        ),
    )(span_order, queries, keys, values, out_weight)


def solution(mesh):
    placed = (P("pp", "cp", "tp"), P("pp", "cp", "tp"), P("pp", "cp", "tp"), P("tp", "cp"), P())
    return jax.shard_map(
        functools.partial(on_device, mesh.shape["pp"], mesh.shape["cp"]),
        mesh=mesh,
        in_specs=placed,
        out_specs=P("pp", None, "tp", "cp"),
        check_vma=False,
    )
```

```python
import functools

import jax
import jax.numpy as jnp
from jax import lax
from jax.experimental import pallas as pl
from jax.experimental.pallas import tpu as pltpu
from jax.sharding import PartitionSpec as P

HEAD = 128
PARTS = 8
EXTRA = 4
FILL = 3
GIFT = 4
AHEAD = 6
OFF1 = 3
OFF2 = 7
OFF3 = 13
OFFG = 6
SIDE_END = 11
SIDE_MID = 10
LAG_END = 5
LAG_MID = 6
TILES = 4
NEAR = True
SPAN = 256
GROUP = 4
MESH = pl.DeviceIdType.MESH


def kernel(
    n_pp,
    n_cp,
    order_in,
    q_ref,
    k_ref,
    v_ref,
    w_ref,
    out_ref,
    order_ref,
    kv,
    qb,
    gs,
    ga,
    wb,
    acc,
    give,
    take,
    mask,
    in_sem,
    order_sem,
    qin_sem,
    w_sem,
    kvs_sem,
    kvx_sem,
    kvr_sem,
    qs_sem,
    qg_sem,
    qr_sem,
    y_sem,
    up_sem,
    down_sem,
    x_sem,
    eu_sem,
    ed_sem,
    g_sem,
    ts_sem,
    tr_sem,
):
    pp, cp, tp = lax.axis_index("pp"), lax.axis_index("cp"), lax.axis_index("tp")
    line = n_cp // 2
    i, x = cp // 2, cp % 2
    side = i * 2 + 1 - x
    rows = kv.shape[2]
    half = rows // 2
    width = qb.shape[3]
    wide = wb.shape[1]
    tile = wide // TILES
    heads = width // HEAD
    after, before = lax.rem(pp + 1, n_pp), lax.rem(pp + n_pp - 1, n_pp)
    right = (pp, side, tp)
    sibling = (pp, cp, 1 - tp)
    has_up, has_down = i + 1 < line, i > 0
    end = (i == 0) | (i == line - 1)
    gift_down, gift_up = i == 1, i == line - 2
    giver = jnp.where(i == 0, 1, line - 2) * 2 + x

    def remote(src, dst, send, recv, device):
        return pltpu.make_async_remote_copy(
            src_ref=src,
            dst_ref=dst,
            send_sem=send,
            recv_sem=recv,
            device_id=device,
            device_id_type=MESH,
        )

    load_k = pltpu.make_async_copy(k_ref.at[0], kv.at[cp, 0], in_sem.at[0])
    load_v = pltpu.make_async_copy(v_ref.at[0], kv.at[cp, 1], in_sem.at[1])
    load_order = pltpu.make_async_copy(order_in, order_ref, order_sem)
    load_k.start()
    load_v.start()
    load_order.start()

    def load_q(s):
        at = pl.ds(pl.multiple_of(s * width, width), width)
        return pltpu.make_async_copy(q_ref.at[0, :, at], qb.at[0, s], qin_sem.at[s])

    @pl.loop(0, PARTS)
    def _(s):
        load_q(s).start()

    load_w = pltpu.make_async_copy(w_ref, wb, w_sem)
    load_w.start()

    barrier = pltpu.get_barrier_semaphore()

    def greet(device):
        pl.semaphore_signal(barrier, inc=1, device_id=device, device_id_type=MESH)

    @pl.loop(0, line)
    def _(j):
        @pl.when(j != i)
        def _():
            greet((pp, j * 2 + x, tp))

    greet((after, cp, tp))
    greet((before, cp, tp))
    greet(right)
    greet(sibling)
    load_k.wait()
    load_v.wait()
    pl.semaphore_wait(barrier, line + 3)

    def kv_line(j, r):
        return remote(kv.at[cp, r], kv.at[cp, r], kvs_sem.at[j, r], kvr_sem.at[cp, r], (pp, j * 2 + x, tp))

    def kv_pass(c, r):
        return remote(kv.at[c, r], kv.at[c, r], kvx_sem.at[c // 2, r], kvr_sem.at[c, r], right)

    def q_side(s):
        return remote(qb.at[0, s], qb.at[1, s], qs_sem, qr_sem.at[0, s], right)

    def q_gift(s, to):
        return remote(qb.at[0, s], qb.at[2, s], qg_sem.at[to], qr_sem.at[1, s], (pp, cp - 2 + 4 * to, tp))

    def in_turn(body):
        @pl.loop(0, line - 1)
        def _(e):
            d = e + 1 if NEAR else line - 1 - e
            for j, inside in ((i - d, i - d >= 0), (i + d, i + d < line)):

                @pl.when(inside)
                def _():
                    body(j)

    @in_turn
    def _(j):
        for r in range(2):
            kv_line(j, r).start()

    for r in range(2):
        kv_pass(cp, r).start()

    @pl.loop(0, PARTS)
    def _(s):
        load_q(s).wait()

        @pl.when(s < FILL)
        def _():
            q_side(s).start()

        for to, there in ((0, gift_down), (1, gift_up)):

            @pl.when(there & (s >= PARTS - GIFT))
            def _():
                q_gift(s, to).start()

    load_order.wait()
    row = lax.broadcasted_iota(jnp.int32, (rows, 1), 0)
    col = lax.broadcasted_iota(jnp.int32, (1, rows), 1)
    for which, block in ((0, cp), (1, side), (2, giver)):
        query_pos = row + jnp.where(row < half, order_ref[2 * block] * half, order_ref[2 * block + 1] * half - half)
        for c in range(n_cp):
            key_pos = col + jnp.where(col < half, order_ref[2 * c] * half, order_ref[2 * c + 1] * half - half)
            mask[which, :, c * rows : (c + 1) * rows] = jnp.where(key_pos <= query_pos, 0.0, -1e30)

    def pass_kv(j):
        for r in range(2):
            kv_pass(j * 2 + x, r).wait_recv()
            kv_pass(j * 2 + x, r).start()

    in_turn(pass_kv)

    @pl.loop(FILL, PARTS)
    def _(s):
        q_side(s).start()

    @pl.loop(0, line)
    def _(j):
        for r in range(2):
            kv_pass(j * 2 + 1 - x, r).wait_recv()

    factor = HEAD ** (-0.5) * 1.4426950408889634
    length = n_cp * rows

    def send_after(which, c, s):
        return remote(gs.at[which, s], ga.at[c, s], y_sem.at[which], g_sem.at[c, s], (after, cp, tp))

    gifts = jnp.where(end, GIFT, 0)

    def attend(a):
        own, gift = a < PARTS, a < PARTS + gifts
        which = jnp.where(own, 0, jnp.where(gift, 2, 1))
        s = a - jnp.where(own, 0, jnp.where(gift, GIFT, PARTS + gifts))

        @pl.when(which == 1)
        def _():
            q_side(s).wait_recv()

        @pl.when(which == 2)
        def _():
            q_gift(s, 0).wait_recv()

        blocks = SPAN // rows
        spans = [(slice(b * blocks, (b + 1) * blocks), slice(b * SPAN, (b + 1) * SPAN)) for b in range(length // SPAN)]

        def scores(h):
            query = qb[which, s, :, h * HEAD : (h + 1) * HEAD]
            return [
                lax.dot_general(
                    query,
                    kv[b, 0].reshape(SPAN, HEAD),
                    (((1,), (1,)), ((), ())),
                    preferred_element_type=jnp.float32,
                )
                + mask[which, :, at]
                for b, at in spans
            ]

        ready = scores(0)
        for h in range(heads):
            score = ready
            if h + 1 < heads:
                ready = scores(h + 1)
            top = jnp.max(functools.reduce(jnp.maximum, score), axis=1, keepdims=True)
            weight = [jnp.exp2((z - top) * factor) for z in score]
            total = jnp.sum(functools.reduce(jnp.add, weight), axis=1, keepdims=True)
            mixed = None
            for (b, _), w in zip(spans, weight):
                term = jnp.dot(
                    w.astype(jnp.bfloat16), kv[b, 1].reshape(SPAN, HEAD), preferred_element_type=jnp.float32
                )
                mixed = term if mixed is None else mixed + term
            gs[which, s, :, h * HEAD : (h + 1) * HEAD] = (mixed / total).astype(jnp.bfloat16)
        send_after(which, jnp.where(own, cp, jnp.where(gift, giver, side)), s).start()

    def send_up(c, s):
        return remote(ga.at[c, s], ga.at[c, s], up_sem.at[c // 2], g_sem.at[c, s], (pp, cp + 2, tp))

    def send_down(c, s):
        return remote(ga.at[c, s], ga.at[c, s], down_sem.at[c // 2], g_sem.at[c, s], (pp, cp - 2, tp))

    def send_side(c, s):
        return remote(ga.at[c, s], ga.at[c, s], x_sem.at[c // 2], g_sem.at[c, s], right)

    def extra_up(s):
        return remote(ga.at[side, s], ga.at[side, s], eu_sem, g_sem.at[side, s], (pp, cp + 2, tp))

    def extra_down(s):
        return remote(ga.at[side, s], ga.at[side, s], ed_sem, g_sem.at[side, s], (pp, cp - 2, tp))

    def swap(c):
        return remote(give.at[c], take.at[c], ts_sem.at[c], tr_sem.at[c], sibling)

    def arrived(c, s):
        send_side(c, s).wait_recv()

    def project(c, p):
        for n in range(TILES):
            cols = slice(n * tile, (n + 1) * tile)
            term = None
            for r in range(GROUP):
                at = pl.ds(pl.multiple_of((GROUP * p + r) * width, width), width)
                piece = jnp.dot(ga[c, GROUP * p + r], wb[at, cols], preferred_element_type=jnp.float32)
                term = piece if term is None else term + piece
            acc[c, :, cols] = jnp.where(p == 0, 0.0, acc[c, :, cols]) + term

    def settle(c):
        theirs = pl.ds(pl.multiple_of((1 - tp) * half, half), half)
        give[c] = acc[c, theirs, :].astype(jnp.bfloat16)
        swap(c).start()

    def finish(c):
        ours = pl.ds(pl.multiple_of(tp * half, half), half)
        swap(c).wait_recv()
        out_ref[0, c] = (acc[c, ours, :] + take[c].astype(jnp.float32)).astype(jnp.bfloat16)

    def consume(c, s):
        project(c, s // GROUP)

        @pl.when(s == PARTS - 1)
        def _():
            settle(c)

    def complete(s):
        return (s & (GROUP - 1)) == GROUP - 1

    @pl.loop(0, AHEAD)
    def _(a):
        attend(a)

    load_w.wait()
    lag = jnp.where(end, LAG_END, LAG_MID)
    side_at = jnp.where(end, SIDE_END, SIDE_MID)
    given = PARTS - GIFT

    def passed(d):
        return jnp.where(d == 0, 0, jnp.where(d == 1, OFF1, jnp.where(d == 2, OFF2, OFF3 + (d - 3) * PARTS))) + PARTS

    last_up = jnp.maximum(passed(i), side_at + PARTS) - 1
    last_down = jnp.maximum(passed(line - 1 - i), side_at + PARTS) - 1
    ticks = max(max(OFF2, OFF3 + (line - 4) * PARTS) + max(LAG_END, LAG_MID), SIDE_END + 3, SIDE_MID + 3) + PARTS

    def by_side(d, s):
        return (d > 1) | (s < PARTS - EXTRA)

    def slot(k, tick):
        if k == 2:
            s = tick - OFFG
            return 1, s, end & (s >= given) & (s < PARTS) & (line > 1)
        since = tick - OFF3 - k * PARTS
        later = since >= 0
        turn = since // (2 * PARTS)
        d = jnp.where(later, 3 + k + 2 * turn, 1 + k)
        s = jnp.where(later, since - turn * (2 * PARTS), tick - (OFF1, OFF2)[k])
        there = (s >= 0) & (s < PARTS) & (d < line)
        if k == 0:
            there &= ~(end & (d == 1) & (s >= given))
        return d, s, there

    def left(ref, sem):
        remote(ref, ref, sem, g_sem.at[0, 0], right).wait_send()

    @pl.loop(0, ticks)
    def _(tick):
        @pl.when(tick < PARTS)
        def _():
            arrived(cp, tick)

            @pl.when(has_up & ~(gift_up & (tick >= given)))
            def _():
                send_up(cp, tick).start()

            @pl.when(has_down & ~(gift_down & (tick >= given)))
            def _():
                send_down(cp, tick).start()

        def relay(d, s):
            @pl.when(i - d >= 0)
            def _():
                c = cp - 2 * d
                arrived(c, s)

                @pl.when(has_up)
                def _():
                    send_up(c, s).start()

                @pl.when(by_side(d, s))
                def _():
                    send_side(c, s).start()

            @pl.when(i + d < line)
            def _():
                c = cp + 2 * d
                arrived(c, s)

                @pl.when(has_down)
                def _():
                    send_down(c, s).start()

                @pl.when(by_side(d, s))
                def _():
                    send_side(c, s).start()

        here = [slot(k, tick) for k in range(3)]
        for d, s, there in here:

            @pl.when(there)
            def _():
                relay(d, s)

        @pl.when(tick + AHEAD < 2 * PARTS + gifts)
        def _():
            attend(tick + AHEAD)

        beside = tick - side_at

        @pl.when((beside >= 0) & (beside < PARTS))
        def _():
            arrived(side, beside)

        @pl.when(has_up & (tick == last_up))
        def _():
            @pl.loop(PARTS - EXTRA, PARTS)
            def _(r):
                extra_up(r).start()

        @pl.when(has_down & (tick == last_down))
        def _():
            @pl.loop(PARTS - EXTRA, PARTS)
            def _(r):
                extra_down(r).start()

        marks = [PARTS + 4, side_at + PARTS + 2, max(OFF1, OFFG) + PARTS + 3, OFF2 + PARTS + 3]

        @pl.when(functools.reduce(jnp.logical_or, [tick == mark for mark in marks]))
        def _():
            @pl.when(tick == PARTS + 4)
            def _():
                finish(cp)

            @pl.when(tick == side_at + PARTS + 2)
            def _():
                finish(side)

            for d, at in ((1, max(OFF1, OFFG)), (2, OFF2)):
                if d < line:

                    @pl.when(tick == at + PARTS + 3)
                    def _():
                        @pl.when(i - d >= 0)
                        def _():
                            finish(cp - 2 * d)

                        @pl.when(i + d < line)
                        def _():
                            finish(cp + 2 * d)

        @pl.when(tick == ticks - 1)
        def _():
            @pl.loop(2, line)
            def _(d):
                @pl.when((i - d >= 0) & (d > 2))
                def _():
                    finish(cp - 2 * d)

                @pl.when((i + d < line) & (d > 2))
                def _():
                    finish(cp + 2 * d)

                @pl.when((i - d >= 0) & (d < line - 1))
                def _():
                    finish(side - 2 * d)

                @pl.when((i + d < line) & (d < line - 1))
                def _():
                    finish(side + 2 * d)

            @in_turn
            def _(j):
                for r in range(2):
                    kv_line(j, r).wait_send()

            @pl.loop(0, line)
            def _(j):
                for r in range(2):
                    kv_pass(j * 2 + x, r).wait_send()

            left(qb.at[0], qs_sem)
            left(gs.at[0], y_sem.at[0])
            left(gs.at[1], y_sem.at[1])

            @pl.when(end)
            def _():
                left(gs.at[2, given:PARTS], y_sem.at[2])

            for to, there in ((0, gift_down), (1, gift_up)):

                @pl.when(there)
                def _():
                    left(qb.at[0, given:PARTS], qg_sem.at[to])

            @pl.loop(PARTS - EXTRA, PARTS)
            def _(r):
                @pl.loop(0, 2)
                def _(far):
                    j = i + 2 * far - 1

                    @pl.when((j >= 0) & (j < line))
                    def _():
                        arrived(j * 2 + 1 - x, r)

                        @pl.when(complete(r))
                        def _():
                            consume(j * 2 + 1 - x, r)

        past = [slot(k, tick - lag) for k in range(3)]
        items = [(0, *item) for item in here] + [(0, 0, tick, tick < PARTS)]
        items += [(1, d, s, there & by_side(d, s)) for d, s, there in past]
        items += [(1, 0, beside, (beside >= 0) & (beside < PARTS))]
        due = [there & complete(s) for _, _, s, there in items]

        @pl.when(functools.reduce(jnp.logical_or, due))
        def _():
            @pl.loop(0, len(items))
            def _(k):
                def pick(values):
                    chosen = values[0]
                    for n, value in enumerate(values[1:], 1):
                        chosen = jnp.where(k == n, value, chosen)
                    return chosen

                @pl.when(pick([flag.astype(jnp.int32) for flag in due]) == 1)
                def _():
                    over = k // 4
                    d, s = pick([item[1] for item in items]), pick([item[2] for item in items])
                    column = jnp.where(over == 1, 1 - x, x)

                    @pl.loop(jnp.where(d == 0, 1, 0), 2)
                    def _(far):
                        j = i + (2 * far - 1) * d
                        c = j * 2 + column

                        @pl.when((j >= 0) & (j < line))
                        def _():
                            @pl.when((over == 1) & (d > 0))
                            def _():
                                @pl.loop(0, GROUP)
                                def _(r):
                                    arrived(c, s - (GROUP - 1) + r)

                            consume(c, s)

    for d in sorted({line - 1, 1}, reverse=True):

        @pl.when(i - d >= 0)
        def _():
            finish(side - 2 * d)

        @pl.when(i + d < line)
        def _():
            finish(side + 2 * d)

    @pl.loop(0, line)
    def _(j):
        c = j * 2 + x
        near = jnp.abs(j - i) == 1

        @pl.when((j != i) & ~near)
        def _():
            left(ga.at[c], x_sem.at[j])

        @pl.when(near)
        def _():
            left(ga.at[c, 0 : PARTS - EXTRA], x_sem.at[j])

        for there, sem, short in (
            ((j <= i) & has_up, up_sem, gift_up & (j == i)),
            ((j >= i) & has_down, down_sem, gift_down & (j == i)),
        ):

            @pl.when(there & short)
            def _():
                left(ga.at[c, 0:given], sem.at[j])

            @pl.when(there & ~short)
            def _():
                left(ga.at[c], sem.at[j])

    @pl.when(has_up)
    def _():
        left(ga.at[side, PARTS - EXTRA : PARTS], eu_sem)

    @pl.when(has_down)
    def _():
        left(ga.at[side, PARTS - EXTRA : PARTS], ed_sem)

    @pl.loop(0, n_cp)
    def _(c):
        swap(c).wait_send()


def on_device(n_pp, n_cp, queries, keys, values, out_weight, span_order):
    rows = queries.shape[1]
    half = rows // 2
    depth, wide = out_weight.shape
    width = depth // PARTS
    line = n_cp // 2
    hbm = pl.BlockSpec(memory_space=pl.ANY)
    dma = pltpu.SemaphoreType.DMA
    queries, keys, values, out_weight, span_order = (
        pltpu.with_memory_space_constraint(a, pltpu.HBM)
        for a in (queries, keys, values, out_weight, span_order)
    )
    return pl.pallas_call(
        functools.partial(kernel, n_pp, n_cp),
        out_shape=pltpu.VMEM((1, n_cp, half, wide), jnp.bfloat16),
        in_specs=[hbm] * 5,
        out_specs=pl.BlockSpec(memory_space=pltpu.VMEM),
        scratch_shapes=[
            pltpu.SMEM(span_order.shape, jnp.int32),
            pltpu.VMEM((n_cp, 2, rows, HEAD), jnp.bfloat16),
            pltpu.VMEM((3, PARTS, rows, width), jnp.bfloat16),
            pltpu.VMEM((3, PARTS, rows, width), jnp.bfloat16),
            pltpu.VMEM((n_cp, PARTS, rows, width), jnp.bfloat16),
            pltpu.VMEM((depth, wide), jnp.bfloat16),
            pltpu.VMEM((n_cp, rows, wide), jnp.float32),
            pltpu.VMEM((n_cp, half, wide), jnp.bfloat16),
            pltpu.VMEM((n_cp, half, wide), jnp.bfloat16),
            pltpu.VMEM((3, rows, n_cp * rows), jnp.float32),
            dma((2,)),
            dma,
            dma((PARTS,)),
            dma,
            dma((line, 2)),
            dma((line, 2)),
            dma((n_cp, 2)),
            dma,
            dma((2,)),
            dma((2, PARTS)),
            dma((3,)),
            dma((line,)),
            dma((line,)),
            dma((line,)),
            dma,
            dma,
            dma((n_cp, PARTS)),
            dma((n_cp,)),
            dma((n_cp,)),
        ],
        compiler_params=pltpu.CompilerParams(
            collective_id=0, has_side_effects=True, vmem_limit_bytes=50000 * 1024
        ),
    )(span_order, queries, keys, values, out_weight)


def solution(mesh):
    placed = (P("pp", "cp", "tp"), P("pp", "cp", "tp"), P("pp", "cp", "tp"), P("tp", "cp"), P())
    return jax.shard_map(
        functools.partial(on_device, mesh.shape["pp"], mesh.shape["cp"]),
        mesh=mesh,
        in_specs=placed,
        out_specs=P("pp", None, "tp", "cp"),
        check_vma=False,
    )
```

```python
import functools

import jax
import jax.numpy as jnp
from jax import lax
from jax.experimental import pallas as pl
from jax.experimental.pallas import tpu as pltpu
from jax.sharding import PartitionSpec as P

HEAD = 128
PARTS = 8
EXTRA = 4
FILL = 1
GIFT = 4
AHEAD = 6
OFF1 = 3
OFF2 = 7
OFF3 = 13
OFFG = 6
SIDE_END = 11
SIDE_MID = 10
LAG_END = 5
LAG_MID = 6
TILES = 4
NEAR = True
SPAN = 256
GROUP = 4
MESH = pl.DeviceIdType.MESH


def kernel(
    n_pp,
    n_cp,
    order_in,
    q_ref,
    k_ref,
    v_ref,
    w_ref,
    out_ref,
    order_ref,
    kv,
    qb,
    gs,
    ga,
    wb,
    acc,
    give,
    take,
    mask,
    in_sem,
    order_sem,
    qin_sem,
    w_sem,
    kvs_sem,
    kvx_sem,
    kvr_sem,
    qs_sem,
    qg_sem,
    qr_sem,
    y_sem,
    up_sem,
    down_sem,
    x_sem,
    eu_sem,
    ed_sem,
    g_sem,
    ts_sem,
    tr_sem,
):
    pp, cp, tp = lax.axis_index("pp"), lax.axis_index("cp"), lax.axis_index("tp")
    line = n_cp // 2
    i, x = cp // 2, cp % 2
    side = i * 2 + 1 - x
    rows = kv.shape[2]
    half = rows // 2
    width = qb.shape[3]
    wide = wb.shape[1]
    tile = wide // TILES
    heads = width // HEAD
    after, before = lax.rem(pp + 1, n_pp), lax.rem(pp + n_pp - 1, n_pp)
    right = (pp, side, tp)
    sibling = (pp, cp, 1 - tp)
    has_up, has_down = i + 1 < line, i > 0
    end = (i == 0) | (i == line - 1)
    gift_down, gift_up = i == 1, i == line - 2
    giver = jnp.where(i == 0, 1, line - 2) * 2 + x

    def remote(src, dst, send, recv, device):
        return pltpu.make_async_remote_copy(
            src_ref=src,
            dst_ref=dst,
            send_sem=send,
            recv_sem=recv,
            device_id=device,
            device_id_type=MESH,
        )

    load_k = pltpu.make_async_copy(k_ref.at[0], kv.at[cp, 0], in_sem.at[0])
    load_v = pltpu.make_async_copy(v_ref.at[0], kv.at[cp, 1], in_sem.at[1])
    load_order = pltpu.make_async_copy(order_in, order_ref, order_sem)
    load_k.start()
    load_v.start()
    load_order.start()

    def load_q(s):
        at = pl.ds(pl.multiple_of(s * width, width), width)
        return pltpu.make_async_copy(q_ref.at[0, :, at], qb.at[0, s], qin_sem.at[s])

    @pl.loop(0, PARTS)
    def _(s):
        load_q(s).start()

    load_w = pltpu.make_async_copy(w_ref, wb, w_sem)
    load_w.start()

    barrier = pltpu.get_barrier_semaphore()

    def greet(device):
        pl.semaphore_signal(barrier, inc=1, device_id=device, device_id_type=MESH)

    @pl.loop(0, line)
    def _(j):
        @pl.when(j != i)
        def _():
            greet((pp, j * 2 + x, tp))

    greet((after, cp, tp))
    greet((before, cp, tp))
    greet(right)
    greet(sibling)
    load_k.wait()
    load_v.wait()
    pl.semaphore_wait(barrier, line + 3)

    def kv_line(j, r):
        return remote(kv.at[cp, r], kv.at[cp, r], kvs_sem.at[j, r], kvr_sem.at[cp, r], (pp, j * 2 + x, tp))

    def kv_pass(c, r):
        return remote(kv.at[c, r], kv.at[c, r], kvx_sem.at[c // 2, r], kvr_sem.at[c, r], right)

    def q_side(s):
        return remote(qb.at[0, s], qb.at[1, s], qs_sem, qr_sem.at[0, s], right)

    def q_gift(s, to):
        return remote(qb.at[0, s], qb.at[2, s], qg_sem.at[to], qr_sem.at[1, s], (pp, cp - 2 + 4 * to, tp))

    def in_turn(body):
        @pl.loop(0, line - 1)
        def _(e):
            d = e + 1 if NEAR else line - 1 - e
            for j, inside in ((i - d, i - d >= 0), (i + d, i + d < line)):

                @pl.when(inside)
                def _():
                    body(j)

    @in_turn
    def _(j):
        for r in range(2):
            kv_line(j, r).start()

    for r in range(2):
        kv_pass(cp, r).start()

    @pl.loop(0, PARTS)
    def _(s):
        load_q(s).wait()

        @pl.when(s < FILL)
        def _():
            q_side(s).start()

    load_order.wait()
    row = lax.broadcasted_iota(jnp.int32, (rows, 1), 0)
    col = lax.broadcasted_iota(jnp.int32, (1, rows), 1)
    for which, block in ((0, cp), (1, side), (2, giver)):
        query_pos = row + jnp.where(row < half, order_ref[2 * block] * half, order_ref[2 * block + 1] * half - half)
        for c in range(n_cp):
            key_pos = col + jnp.where(col < half, order_ref[2 * c] * half, order_ref[2 * c + 1] * half - half)
            mask[which, :, c * rows : (c + 1) * rows] = jnp.where(key_pos <= query_pos, 0.0, -1e30)

    def pass_kv(j):
        for r in range(2):
            kv_pass(j * 2 + x, r).wait_recv()
            kv_pass(j * 2 + x, r).start()

    in_turn(pass_kv)

    for to, there in ((0, gift_down), (1, gift_up)):

        @pl.when(there)
        def _():
            @pl.loop(PARTS - GIFT, PARTS)
            def _(s):
                q_gift(s, to).start()

    @pl.loop(FILL, PARTS)
    def _(s):
        q_side(s).start()

    @pl.loop(0, line)
    def _(j):
        for r in range(2):
            kv_pass(j * 2 + 1 - x, r).wait_recv()

    factor = HEAD ** (-0.5) * 1.4426950408889634
    length = n_cp * rows

    def send_after(which, c, s):
        return remote(gs.at[which, s], ga.at[c, s], y_sem.at[which], g_sem.at[c, s], (after, cp, tp))

    gifts = jnp.where(end, GIFT, 0)

    def attend(a):
        own, gift = a < PARTS, a < PARTS + gifts
        which = jnp.where(own, 0, jnp.where(gift, 2, 1))
        s = a - jnp.where(own, 0, jnp.where(gift, GIFT, PARTS + gifts))

        @pl.when(which == 1)
        def _():
            q_side(s).wait_recv()

        @pl.when(which == 2)
        def _():
            q_gift(s, 0).wait_recv()

        blocks = SPAN // rows
        spans = [(slice(b * blocks, (b + 1) * blocks), slice(b * SPAN, (b + 1) * SPAN)) for b in range(length // SPAN)]

        def scores(h):
            query = qb[which, s, :, h * HEAD : (h + 1) * HEAD]
            return [
                lax.dot_general(
                    query,
                    kv[b, 0].reshape(SPAN, HEAD),
                    (((1,), (1,)), ((), ())),
                    preferred_element_type=jnp.float32,
                )
                + mask[which, :, at]
                for b, at in spans
            ]

        ready = scores(0)
        for h in range(heads):
            score = ready
            if h + 1 < heads:
                ready = scores(h + 1)
            top = jnp.max(functools.reduce(jnp.maximum, score), axis=1, keepdims=True)
            weight = [jnp.exp2((z - top) * factor) for z in score]
            total = jnp.sum(functools.reduce(jnp.add, weight), axis=1, keepdims=True)
            mixed = None
            for (b, _), w in zip(spans, weight):
                term = jnp.dot(
                    w.astype(jnp.bfloat16), kv[b, 1].reshape(SPAN, HEAD), preferred_element_type=jnp.float32
                )
                mixed = term if mixed is None else mixed + term
            gs[which, s, :, h * HEAD : (h + 1) * HEAD] = (mixed / total).astype(jnp.bfloat16)
        send_after(which, jnp.where(own, cp, jnp.where(gift, giver, side)), s).start()

    def send_up(c, s):
        return remote(ga.at[c, s], ga.at[c, s], up_sem.at[c // 2], g_sem.at[c, s], (pp, cp + 2, tp))

    def send_down(c, s):
        return remote(ga.at[c, s], ga.at[c, s], down_sem.at[c // 2], g_sem.at[c, s], (pp, cp - 2, tp))

    def send_side(c, s):
        return remote(ga.at[c, s], ga.at[c, s], x_sem.at[c // 2], g_sem.at[c, s], right)

    def extra_up(s):
        return remote(ga.at[side, s], ga.at[side, s], eu_sem, g_sem.at[side, s], (pp, cp + 2, tp))

    def extra_down(s):
        return remote(ga.at[side, s], ga.at[side, s], ed_sem, g_sem.at[side, s], (pp, cp - 2, tp))

    def swap(c):
        return remote(give.at[c], take.at[c], ts_sem.at[c], tr_sem.at[c], sibling)

    def arrived(c, s):
        send_side(c, s).wait_recv()

    def project(c, p):
        for n in range(TILES):
            cols = slice(n * tile, (n + 1) * tile)
            term = None
            for r in range(GROUP):
                at = pl.ds(pl.multiple_of((GROUP * p + r) * width, width), width)
                piece = jnp.dot(ga[c, GROUP * p + r], wb[at, cols], preferred_element_type=jnp.float32)
                term = piece if term is None else term + piece
            acc[c, :, cols] = jnp.where(p == 0, 0.0, acc[c, :, cols]) + term

    def settle(c):
        theirs = pl.ds(pl.multiple_of((1 - tp) * half, half), half)
        give[c] = acc[c, theirs, :].astype(jnp.bfloat16)
        swap(c).start()

    def finish(c):
        ours = pl.ds(pl.multiple_of(tp * half, half), half)
        swap(c).wait_recv()
        out_ref[0, c] = (acc[c, ours, :] + take[c].astype(jnp.float32)).astype(jnp.bfloat16)

    def consume(c, s):
        project(c, s // GROUP)

        @pl.when(s == PARTS - 1)
        def _():
            settle(c)

    def complete(s):
        return (s & (GROUP - 1)) == GROUP - 1

    @pl.loop(0, AHEAD)
    def _(a):
        attend(a)

    load_w.wait()
    lag = jnp.where(end, LAG_END, LAG_MID)
    side_at = jnp.where(end, SIDE_END, SIDE_MID)
    given = PARTS - GIFT

    def passed(d):
        return jnp.where(d == 0, 0, jnp.where(d == 1, OFF1, jnp.where(d == 2, OFF2, OFF3 + (d - 3) * PARTS))) + PARTS

    last_up = jnp.maximum(passed(i), side_at + PARTS) - 1
    last_down = jnp.maximum(passed(line - 1 - i), side_at + PARTS) - 1
    ticks = max(max(OFF2, OFF3 + (line - 4) * PARTS) + max(LAG_END, LAG_MID), SIDE_END + 3, SIDE_MID + 3) + PARTS

    def by_side(d, s):
        return (d > 1) | (s < PARTS - EXTRA)

    def slot(k, tick):
        if k == 2:
            s = tick - OFFG
            return 1, s, end & (s >= given) & (s < PARTS) & (line > 1)
        since = tick - OFF3 - k * PARTS
        later = since >= 0
        turn = since // (2 * PARTS)
        d = jnp.where(later, 3 + k + 2 * turn, 1 + k)
        s = jnp.where(later, since - turn * (2 * PARTS), tick - (OFF1, OFF2)[k])
        there = (s >= 0) & (s < PARTS) & (d < line)
        if k == 0:
            there &= ~(end & (d == 1) & (s >= given))
        return d, s, there

    def left(ref, sem):
        remote(ref, ref, sem, g_sem.at[0, 0], right).wait_send()

    @pl.loop(0, ticks)
    def _(tick):
        @pl.when(tick < PARTS)
        def _():
            arrived(cp, tick)

            @pl.when(has_up & ~(gift_up & (tick >= given)))
            def _():
                send_up(cp, tick).start()

            @pl.when(has_down & ~(gift_down & (tick >= given)))
            def _():
                send_down(cp, tick).start()

        def relay(d, s):
            @pl.when(i - d >= 0)
            def _():
                c = cp - 2 * d
                arrived(c, s)

                @pl.when(has_up)
                def _():
                    send_up(c, s).start()

                @pl.when(by_side(d, s))
                def _():
                    send_side(c, s).start()

            @pl.when(i + d < line)
            def _():
                c = cp + 2 * d
                arrived(c, s)

                @pl.when(has_down)
                def _():
                    send_down(c, s).start()

                @pl.when(by_side(d, s))
                def _():
                    send_side(c, s).start()

        here = [slot(k, tick) for k in range(3)]
        for d, s, there in here:

            @pl.when(there)
            def _():
                relay(d, s)

        @pl.when(tick + AHEAD < 2 * PARTS + gifts)
        def _():
            attend(tick + AHEAD)

        beside = tick - side_at

        @pl.when((beside >= 0) & (beside < PARTS))
        def _():
            arrived(side, beside)

        @pl.when(has_up & (tick == last_up))
        def _():
            @pl.loop(PARTS - EXTRA, PARTS)
            def _(r):
                extra_up(r).start()

        @pl.when(has_down & (tick == last_down))
        def _():
            @pl.loop(PARTS - EXTRA, PARTS)
            def _(r):
                extra_down(r).start()

        marks = [PARTS + 4, side_at + PARTS + 2, max(OFF1, OFFG) + PARTS + 3, OFF2 + PARTS + 3]

        @pl.when(functools.reduce(jnp.logical_or, [tick == mark for mark in marks]))
        def _():
            @pl.when(tick == PARTS + 4)
            def _():
                finish(cp)

            @pl.when(tick == side_at + PARTS + 2)
            def _():
                finish(side)

            for d, at in ((1, max(OFF1, OFFG)), (2, OFF2)):
                if d < line:

                    @pl.when(tick == at + PARTS + 3)
                    def _():
                        @pl.when(i - d >= 0)
                        def _():
                            finish(cp - 2 * d)

                        @pl.when(i + d < line)
                        def _():
                            finish(cp + 2 * d)

        @pl.when(tick == ticks - 1)
        def _():
            @pl.loop(2, line)
            def _(d):
                @pl.when((i - d >= 0) & (d > 2))
                def _():
                    finish(cp - 2 * d)

                @pl.when((i + d < line) & (d > 2))
                def _():
                    finish(cp + 2 * d)

                @pl.when((i - d >= 0) & (d < line - 1))
                def _():
                    finish(side - 2 * d)

                @pl.when((i + d < line) & (d < line - 1))
                def _():
                    finish(side + 2 * d)

            @in_turn
            def _(j):
                for r in range(2):
                    kv_line(j, r).wait_send()

            @pl.loop(0, line)
            def _(j):
                for r in range(2):
                    kv_pass(j * 2 + x, r).wait_send()

            left(qb.at[0], qs_sem)
            left(gs.at[0], y_sem.at[0])
            left(gs.at[1], y_sem.at[1])

            @pl.when(end)
            def _():
                left(gs.at[2, given:PARTS], y_sem.at[2])

            for to, there in ((0, gift_down), (1, gift_up)):

                @pl.when(there)
                def _():
                    left(qb.at[0, given:PARTS], qg_sem.at[to])

            @pl.loop(PARTS - EXTRA, PARTS)
            def _(r):
                @pl.loop(0, 2)
                def _(far):
                    j = i + 2 * far - 1

                    @pl.when((j >= 0) & (j < line))
                    def _():
                        arrived(j * 2 + 1 - x, r)

                        @pl.when(complete(r))
                        def _():
                            consume(j * 2 + 1 - x, r)

        past = [slot(k, tick - lag) for k in range(3)]
        items = [(0, *item) for item in here] + [(0, 0, tick, tick < PARTS)]
        items += [(1, d, s, there & by_side(d, s)) for d, s, there in past]
        items += [(1, 0, beside, (beside >= 0) & (beside < PARTS))]
        due = [there & complete(s) for _, _, s, there in items]

        @pl.when(functools.reduce(jnp.logical_or, due))
        def _():
            @pl.loop(0, len(items))
            def _(k):
                def pick(values):
                    chosen = values[0]
                    for n, value in enumerate(values[1:], 1):
                        chosen = jnp.where(k == n, value, chosen)
                    return chosen

                @pl.when(pick([flag.astype(jnp.int32) for flag in due]) == 1)
                def _():
                    over = k // 4
                    d, s = pick([item[1] for item in items]), pick([item[2] for item in items])
                    column = jnp.where(over == 1, 1 - x, x)

                    @pl.loop(jnp.where(d == 0, 1, 0), 2)
                    def _(far):
                        j = i + (2 * far - 1) * d
                        c = j * 2 + column

                        @pl.when((j >= 0) & (j < line))
                        def _():
                            @pl.when((over == 1) & (d > 0))
                            def _():
                                @pl.loop(0, GROUP)
                                def _(r):
                                    arrived(c, s - (GROUP - 1) + r)

                            consume(c, s)

    for d in sorted({line - 1, 1}, reverse=True):

        @pl.when(i - d >= 0)
        def _():
            finish(side - 2 * d)

        @pl.when(i + d < line)
        def _():
            finish(side + 2 * d)

    @pl.loop(0, line)
    def _(j):
        c = j * 2 + x
        near = jnp.abs(j - i) == 1

        @pl.when((j != i) & ~near)
        def _():
            left(ga.at[c], x_sem.at[j])

        @pl.when(near)
        def _():
            left(ga.at[c, 0 : PARTS - EXTRA], x_sem.at[j])

        for there, sem, short in (
            ((j <= i) & has_up, up_sem, gift_up & (j == i)),
            ((j >= i) & has_down, down_sem, gift_down & (j == i)),
        ):

            @pl.when(there & short)
            def _():
                left(ga.at[c, 0:given], sem.at[j])

            @pl.when(there & ~short)
            def _():
                left(ga.at[c], sem.at[j])

    @pl.when(has_up)
    def _():
        left(ga.at[side, PARTS - EXTRA : PARTS], eu_sem)

    @pl.when(has_down)
    def _():
        left(ga.at[side, PARTS - EXTRA : PARTS], ed_sem)

    @pl.loop(0, n_cp)
    def _(c):
        swap(c).wait_send()


def on_device(n_pp, n_cp, queries, keys, values, out_weight, span_order):
    rows = queries.shape[1]
    half = rows // 2
    depth, wide = out_weight.shape
    width = depth // PARTS
    line = n_cp // 2
    hbm = pl.BlockSpec(memory_space=pl.ANY)
    dma = pltpu.SemaphoreType.DMA
    queries, keys, values, out_weight, span_order = (
        pltpu.with_memory_space_constraint(a, pltpu.HBM)
        for a in (queries, keys, values, out_weight, span_order)
    )
    return pl.pallas_call(
        functools.partial(kernel, n_pp, n_cp),
        out_shape=pltpu.VMEM((1, n_cp, half, wide), jnp.bfloat16),
        in_specs=[hbm] * 5,
        out_specs=pl.BlockSpec(memory_space=pltpu.VMEM),
        scratch_shapes=[
            pltpu.SMEM(span_order.shape, jnp.int32),
            pltpu.VMEM((n_cp, 2, rows, HEAD), jnp.bfloat16),
            pltpu.VMEM((3, PARTS, rows, width), jnp.bfloat16),
            pltpu.VMEM((3, PARTS, rows, width), jnp.bfloat16),
            pltpu.VMEM((n_cp, PARTS, rows, width), jnp.bfloat16),
            pltpu.VMEM((depth, wide), jnp.bfloat16),
            pltpu.VMEM((n_cp, rows, wide), jnp.float32),
            pltpu.VMEM((n_cp, half, wide), jnp.bfloat16),
            pltpu.VMEM((n_cp, half, wide), jnp.bfloat16),
            pltpu.VMEM((3, rows, n_cp * rows), jnp.float32),
            dma((2,)),
            dma,
            dma((PARTS,)),
            dma,
            dma((line, 2)),
            dma((line, 2)),
            dma((n_cp, 2)),
            dma,
            dma((2,)),
            dma((2, PARTS)),
            dma((3,)),
            dma((line,)),
            dma((line,)),
            dma((line,)),
            dma,
            dma,
            dma((n_cp, PARTS)),
            dma((n_cp,)),
            dma((n_cp,)),
        ],
        compiler_params=pltpu.CompilerParams(
            collective_id=0, has_side_effects=True, vmem_limit_bytes=50000 * 1024
        ),
    )(span_order, queries, keys, values, out_weight)


def solution(mesh):
    placed = (P("pp", "cp", "tp"), P("pp", "cp", "tp"), P("pp", "cp", "tp"), P("tp", "cp"), P())
    return jax.shard_map(
        functools.partial(on_device, mesh.shape["pp"], mesh.shape["cp"]),
        mesh=mesh,
        in_specs=placed,
        out_specs=P("pp", None, "tp", "cp"),
        check_vma=False,
    )
```

```python
import functools

import jax
import jax.numpy as jnp
from jax import lax
from jax.experimental import pallas as pl
from jax.experimental.pallas import tpu as pltpu
from jax.sharding import PartitionSpec as P

HEAD = 128
PARTS = 8
EXTRA = 4
FILL = 1
GIFT = 4
AHEAD = 6
OFF1 = 3
OFF2 = 7
OFF3 = 13
OFFG = 6
SIDE_END = 11
SIDE_MID = 10
LAG_END = 5
LAG_MID = 6
TILES = 8
NEAR = True
SPAN = 256
GROUP = 4
MESH = pl.DeviceIdType.MESH


def kernel(
    n_pp,
    n_cp,
    order_in,
    q_ref,
    k_ref,
    v_ref,
    w_ref,
    out_ref,
    order_ref,
    kv,
    qb,
    gs,
    ga,
    wb,
    acc,
    give,
    take,
    mask,
    in_sem,
    order_sem,
    qin_sem,
    w_sem,
    kvs_sem,
    kvx_sem,
    kvr_sem,
    qs_sem,
    qg_sem,
    qr_sem,
    y_sem,
    up_sem,
    down_sem,
    x_sem,
    eu_sem,
    ed_sem,
    g_sem,
    ts_sem,
    tr_sem,
):
    pp, cp, tp = lax.axis_index("pp"), lax.axis_index("cp"), lax.axis_index("tp")
    line = n_cp // 2
    i, x = cp // 2, cp % 2
    side = i * 2 + 1 - x
    rows = kv.shape[2]
    half = rows // 2
    width = qb.shape[3]
    wide = wb.shape[1]
    tile = wide // TILES
    heads = width // HEAD
    after, before = lax.rem(pp + 1, n_pp), lax.rem(pp + n_pp - 1, n_pp)
    right = (pp, side, tp)
    sibling = (pp, cp, 1 - tp)
    has_up, has_down = i + 1 < line, i > 0
    end = (i == 0) | (i == line - 1)
    gift_down, gift_up = i == 1, i == line - 2
    giver = jnp.where(i == 0, 1, line - 2) * 2 + x

    def remote(src, dst, send, recv, device):
        return pltpu.make_async_remote_copy(
            src_ref=src,
            dst_ref=dst,
            send_sem=send,
            recv_sem=recv,
            device_id=device,
            device_id_type=MESH,
        )

    load_k = pltpu.make_async_copy(k_ref.at[0], kv.at[cp, 0], in_sem.at[0])
    load_v = pltpu.make_async_copy(v_ref.at[0], kv.at[cp, 1], in_sem.at[1])
    load_order = pltpu.make_async_copy(order_in, order_ref, order_sem)
    load_k.start()
    load_v.start()
    load_order.start()

    def load_q(s):
        at = pl.ds(pl.multiple_of(s * width, width), width)
        return pltpu.make_async_copy(q_ref.at[0, :, at], qb.at[0, s], qin_sem.at[s])

    @pl.loop(0, PARTS)
    def _(s):
        load_q(s).start()

    load_w = pltpu.make_async_copy(w_ref, wb, w_sem)
    load_w.start()

    barrier = pltpu.get_barrier_semaphore()

    def greet(device):
        pl.semaphore_signal(barrier, inc=1, device_id=device, device_id_type=MESH)

    @pl.loop(0, line)
    def _(j):
        @pl.when(j != i)
        def _():
            greet((pp, j * 2 + x, tp))

    greet((after, cp, tp))
    greet((before, cp, tp))
    greet(right)
    greet(sibling)
    load_k.wait()
    load_v.wait()
    pl.semaphore_wait(barrier, line + 3)

    def kv_line(j, r):
        return remote(kv.at[cp, r], kv.at[cp, r], kvs_sem.at[j, r], kvr_sem.at[cp, r], (pp, j * 2 + x, tp))

    def kv_pass(c, r):
        return remote(kv.at[c, r], kv.at[c, r], kvx_sem.at[c // 2, r], kvr_sem.at[c, r], right)

    def q_side(s):
        return remote(qb.at[0, s], qb.at[1, s], qs_sem, qr_sem.at[0, s], right)

    def q_gift(s, to):
        return remote(qb.at[0, s], qb.at[2, s], qg_sem.at[to], qr_sem.at[1, s], (pp, cp - 2 + 4 * to, tp))

    def in_turn(body):
        @pl.loop(0, line - 1)
        def _(e):
            d = e + 1 if NEAR else line - 1 - e
            for j, inside in ((i - d, i - d >= 0), (i + d, i + d < line)):

                @pl.when(inside)
                def _():
                    body(j)

    @in_turn
    def _(j):
        for r in range(2):
            kv_line(j, r).start()

    for r in range(2):
        kv_pass(cp, r).start()

    @pl.loop(0, PARTS)
    def _(s):
        load_q(s).wait()

        @pl.when(s < FILL)
        def _():
            q_side(s).start()

    load_order.wait()
    row = lax.broadcasted_iota(jnp.int32, (rows, 1), 0)
    col = lax.broadcasted_iota(jnp.int32, (1, rows), 1)
    for which, block in ((0, cp), (1, side), (2, giver)):
        query_pos = row + jnp.where(row < half, order_ref[2 * block] * half, order_ref[2 * block + 1] * half - half)
        for c in range(n_cp):
            key_pos = col + jnp.where(col < half, order_ref[2 * c] * half, order_ref[2 * c + 1] * half - half)
            mask[which, :, c * rows : (c + 1) * rows] = jnp.where(key_pos <= query_pos, 0.0, -1e30)

    def pass_kv(j):
        for r in range(2):
            kv_pass(j * 2 + x, r).wait_recv()
            kv_pass(j * 2 + x, r).start()

    in_turn(pass_kv)

    for to, there in ((0, gift_down), (1, gift_up)):

        @pl.when(there)
        def _():
            @pl.loop(PARTS - GIFT, PARTS)
            def _(s):
                q_gift(s, to).start()

    @pl.loop(FILL, PARTS)
    def _(s):
        q_side(s).start()

    @pl.loop(0, line)
    def _(j):
        for r in range(2):
            kv_pass(j * 2 + 1 - x, r).wait_recv()

    factor = HEAD ** (-0.5) * 1.4426950408889634
    length = n_cp * rows

    def send_after(which, c, s):
        return remote(gs.at[which, s], ga.at[c, s], y_sem.at[which], g_sem.at[c, s], (after, cp, tp))

    gifts = jnp.where(end, GIFT, 0)

    def attend(a):
        own, gift = a < PARTS, a < PARTS + gifts
        which = jnp.where(own, 0, jnp.where(gift, 2, 1))
        s = a - jnp.where(own, 0, jnp.where(gift, GIFT, PARTS + gifts))

        @pl.when(which == 1)
        def _():
            q_side(s).wait_recv()

        @pl.when(which == 2)
        def _():
            q_gift(s, 0).wait_recv()

        blocks = SPAN // rows
        spans = [(slice(b * blocks, (b + 1) * blocks), slice(b * SPAN, (b + 1) * SPAN)) for b in range(length // SPAN)]

        def scores(h):
            query = qb[which, s, :, h * HEAD : (h + 1) * HEAD]
            return [
                lax.dot_general(
                    query,
                    kv[b, 0].reshape(SPAN, HEAD),
                    (((1,), (1,)), ((), ())),
                    preferred_element_type=jnp.float32,
                )
                + mask[which, :, at]
                for b, at in spans
            ]

        ready = scores(0)
        for h in range(heads):
            score = ready
            if h + 1 < heads:
                ready = scores(h + 1)
            top = jnp.max(functools.reduce(jnp.maximum, score), axis=1, keepdims=True)
            weight = [jnp.exp2((z - top) * factor) for z in score]
            total = jnp.sum(functools.reduce(jnp.add, weight), axis=1, keepdims=True)
            mixed = None
            for (b, _), w in zip(spans, weight):
                term = jnp.dot(
                    w.astype(jnp.bfloat16), kv[b, 1].reshape(SPAN, HEAD), preferred_element_type=jnp.float32
                )
                mixed = term if mixed is None else mixed + term
            gs[which, s, :, h * HEAD : (h + 1) * HEAD] = (mixed / total).astype(jnp.bfloat16)
        send_after(which, jnp.where(own, cp, jnp.where(gift, giver, side)), s).start()

    def send_up(c, s):
        return remote(ga.at[c, s], ga.at[c, s], up_sem.at[c // 2], g_sem.at[c, s], (pp, cp + 2, tp))

    def send_down(c, s):
        return remote(ga.at[c, s], ga.at[c, s], down_sem.at[c // 2], g_sem.at[c, s], (pp, cp - 2, tp))

    def send_side(c, s):
        return remote(ga.at[c, s], ga.at[c, s], x_sem.at[c // 2], g_sem.at[c, s], right)

    def extra_up(s):
        return remote(ga.at[side, s], ga.at[side, s], eu_sem, g_sem.at[side, s], (pp, cp + 2, tp))

    def extra_down(s):
        return remote(ga.at[side, s], ga.at[side, s], ed_sem, g_sem.at[side, s], (pp, cp - 2, tp))

    def swap(c):
        return remote(give.at[c], take.at[c], ts_sem.at[c], tr_sem.at[c], sibling)

    def arrived(c, s):
        send_side(c, s).wait_recv()

    def project(c, p):
        for n in range(TILES):
            cols = slice(n * tile, (n + 1) * tile)
            term = None
            for r in range(GROUP):
                at = pl.ds(pl.multiple_of((GROUP * p + r) * width, width), width)
                piece = jnp.dot(ga[c, GROUP * p + r], wb[at, cols], preferred_element_type=jnp.float32)
                term = piece if term is None else term + piece
            acc[c, :, cols] = jnp.where(p == 0, 0.0, acc[c, :, cols]) + term

    def settle(c):
        theirs = pl.ds(pl.multiple_of((1 - tp) * half, half), half)
        give[c] = acc[c, theirs, :].astype(jnp.bfloat16)
        swap(c).start()

    def finish(c):
        ours = pl.ds(pl.multiple_of(tp * half, half), half)
        swap(c).wait_recv()
        out_ref[0, c] = (acc[c, ours, :] + take[c].astype(jnp.float32)).astype(jnp.bfloat16)

    def consume(c, s):
        project(c, s // GROUP)

        @pl.when(s == PARTS - 1)
        def _():
            settle(c)

    def complete(s):
        return (s & (GROUP - 1)) == GROUP - 1

    @pl.loop(0, AHEAD)
    def _(a):
        attend(a)

    load_w.wait()
    lag = jnp.where(end, LAG_END, LAG_MID)
    side_at = jnp.where(end, SIDE_END, SIDE_MID)
    given = PARTS - GIFT

    def passed(d):
        return jnp.where(d == 0, 0, jnp.where(d == 1, OFF1, jnp.where(d == 2, OFF2, OFF3 + (d - 3) * PARTS))) + PARTS

    last_up = jnp.maximum(passed(i), side_at + PARTS) - 1
    last_down = jnp.maximum(passed(line - 1 - i), side_at + PARTS) - 1
    ticks = max(max(OFF2, OFF3 + (line - 4) * PARTS) + max(LAG_END, LAG_MID), SIDE_END + 3, SIDE_MID + 3) + PARTS

    def by_side(d, s):
        return (d > 1) | (s < PARTS - EXTRA)

    def slot(k, tick):
        if k == 2:
            s = tick - OFFG
            return 1, s, end & (s >= given) & (s < PARTS) & (line > 1)
        since = tick - OFF3 - k * PARTS
        later = since >= 0
        turn = since // (2 * PARTS)
        d = jnp.where(later, 3 + k + 2 * turn, 1 + k)
        s = jnp.where(later, since - turn * (2 * PARTS), tick - (OFF1, OFF2)[k])
        there = (s >= 0) & (s < PARTS) & (d < line)
        if k == 0:
            there &= ~(end & (d == 1) & (s >= given))
        return d, s, there

    def left(ref, sem):
        remote(ref, ref, sem, g_sem.at[0, 0], right).wait_send()

    @pl.loop(0, ticks)
    def _(tick):
        @pl.when(tick < PARTS)
        def _():
            arrived(cp, tick)

            @pl.when(has_up & ~(gift_up & (tick >= given)))
            def _():
                send_up(cp, tick).start()

            @pl.when(has_down & ~(gift_down & (tick >= given)))
            def _():
                send_down(cp, tick).start()

        def relay(d, s):
            @pl.when(i - d >= 0)
            def _():
                c = cp - 2 * d
                arrived(c, s)

                @pl.when(by_side(d, s))
                def _():
                    send_side(c, s).start()

                @pl.when(has_up)
                def _():
                    send_up(c, s).start()

            @pl.when(i + d < line)
            def _():
                c = cp + 2 * d
                arrived(c, s)

                @pl.when(by_side(d, s))
                def _():
                    send_side(c, s).start()

                @pl.when(has_down)
                def _():
                    send_down(c, s).start()

        here = [slot(k, tick) for k in range(3)]
        for d, s, there in here:

            @pl.when(there)
            def _():
                relay(d, s)

        @pl.when(tick + AHEAD < 2 * PARTS + gifts)
        def _():
            attend(tick + AHEAD)

        beside = tick - side_at

        @pl.when((beside >= 0) & (beside < PARTS))
        def _():
            arrived(side, beside)

        @pl.when(has_up & (tick == last_up))
        def _():
            @pl.loop(PARTS - EXTRA, PARTS)
            def _(r):
                extra_up(r).start()

        @pl.when(has_down & (tick == last_down))
        def _():
            @pl.loop(PARTS - EXTRA, PARTS)
            def _(r):
                extra_down(r).start()

        marks = [PARTS + 4, side_at + PARTS + 2, max(OFF1, OFFG) + PARTS + 3, OFF2 + PARTS + 3]

        @pl.when(functools.reduce(jnp.logical_or, [tick == mark for mark in marks]))
        def _():
            @pl.when(tick == PARTS + 4)
            def _():
                finish(cp)

            @pl.when(tick == side_at + PARTS + 2)
            def _():
                finish(side)

            for d, at in ((1, max(OFF1, OFFG)), (2, OFF2)):
                if d < line:

                    @pl.when(tick == at + PARTS + 3)
                    def _():
                        @pl.when(i - d >= 0)
                        def _():
                            finish(cp - 2 * d)

                        @pl.when(i + d < line)
                        def _():
                            finish(cp + 2 * d)

        @pl.when(tick == ticks - 1)
        def _():
            @pl.loop(2, line)
            def _(d):
                @pl.when((i - d >= 0) & (d > 2))
                def _():
                    finish(cp - 2 * d)

                @pl.when((i + d < line) & (d > 2))
                def _():
                    finish(cp + 2 * d)

                @pl.when((i - d >= 0) & (d < line - 1))
                def _():
                    finish(side - 2 * d)

                @pl.when((i + d < line) & (d < line - 1))
                def _():
                    finish(side + 2 * d)

            @in_turn
            def _(j):
                for r in range(2):
                    kv_line(j, r).wait_send()

            @pl.loop(0, line)
            def _(j):
                for r in range(2):
                    kv_pass(j * 2 + x, r).wait_send()

            left(qb.at[0], qs_sem)
            left(gs.at[0], y_sem.at[0])
            left(gs.at[1], y_sem.at[1])

            @pl.when(end)
            def _():
                left(gs.at[2, given:PARTS], y_sem.at[2])

            for to, there in ((0, gift_down), (1, gift_up)):

                @pl.when(there)
                def _():
                    left(qb.at[0, given:PARTS], qg_sem.at[to])

            @pl.loop(PARTS - EXTRA, PARTS)
            def _(r):
                @pl.loop(0, 2)
                def _(far):
                    j = i + 2 * far - 1

                    @pl.when((j >= 0) & (j < line))
                    def _():
                        arrived(j * 2 + 1 - x, r)

                        @pl.when(complete(r))
                        def _():
                            consume(j * 2 + 1 - x, r)

        past = [slot(k, tick - lag) for k in range(3)]
        items = [(0, *item) for item in here] + [(0, 0, tick, tick < PARTS)]
        items += [(1, d, s, there & by_side(d, s)) for d, s, there in past]
        items += [(1, 0, beside, (beside >= 0) & (beside < PARTS))]
        due = [there & complete(s) for _, _, s, there in items]

        @pl.when(functools.reduce(jnp.logical_or, due))
        def _():
            @pl.loop(0, len(items))
            def _(k):
                def pick(values):
                    chosen = values[0]
                    for n, value in enumerate(values[1:], 1):
                        chosen = jnp.where(k == n, value, chosen)
                    return chosen

                @pl.when(pick([flag.astype(jnp.int32) for flag in due]) == 1)
                def _():
                    over = k // 4
                    d, s = pick([item[1] for item in items]), pick([item[2] for item in items])
                    column = jnp.where(over == 1, 1 - x, x)

                    @pl.loop(jnp.where(d == 0, 1, 0), 2)
                    def _(far):
                        j = i + (2 * far - 1) * d
                        c = j * 2 + column

                        @pl.when((j >= 0) & (j < line))
                        def _():
                            @pl.when((over == 1) & (d > 0))
                            def _():
                                @pl.loop(0, GROUP)
                                def _(r):
                                    arrived(c, s - (GROUP - 1) + r)

                            consume(c, s)

    for d in sorted({line - 1, 1}, reverse=True):

        @pl.when(i - d >= 0)
        def _():
            finish(side - 2 * d)

        @pl.when(i + d < line)
        def _():
            finish(side + 2 * d)

    @pl.loop(0, line)
    def _(j):
        c = j * 2 + x
        near = jnp.abs(j - i) == 1

        @pl.when((j != i) & ~near)
        def _():
            left(ga.at[c], x_sem.at[j])

        @pl.when(near)
        def _():
            left(ga.at[c, 0 : PARTS - EXTRA], x_sem.at[j])

        for there, sem, short in (
            ((j <= i) & has_up, up_sem, gift_up & (j == i)),
            ((j >= i) & has_down, down_sem, gift_down & (j == i)),
        ):

            @pl.when(there & short)
            def _():
                left(ga.at[c, 0:given], sem.at[j])

            @pl.when(there & ~short)
            def _():
                left(ga.at[c], sem.at[j])

    @pl.when(has_up)
    def _():
        left(ga.at[side, PARTS - EXTRA : PARTS], eu_sem)

    @pl.when(has_down)
    def _():
        left(ga.at[side, PARTS - EXTRA : PARTS], ed_sem)

    @pl.loop(0, n_cp)
    def _(c):
        swap(c).wait_send()


def on_device(n_pp, n_cp, queries, keys, values, out_weight, span_order):
    rows = queries.shape[1]
    half = rows // 2
    depth, wide = out_weight.shape
    width = depth // PARTS
    line = n_cp // 2
    hbm = pl.BlockSpec(memory_space=pl.ANY)
    dma = pltpu.SemaphoreType.DMA
    queries, keys, values, out_weight, span_order = (
        pltpu.with_memory_space_constraint(a, pltpu.HBM)
        for a in (queries, keys, values, out_weight, span_order)
    )
    return pl.pallas_call(
        functools.partial(kernel, n_pp, n_cp),
        out_shape=pltpu.VMEM((1, n_cp, half, wide), jnp.bfloat16),
        in_specs=[hbm] * 5,
        out_specs=pl.BlockSpec(memory_space=pltpu.VMEM),
        scratch_shapes=[
            pltpu.SMEM(span_order.shape, jnp.int32),
            pltpu.VMEM((n_cp, 2, rows, HEAD), jnp.bfloat16),
            pltpu.VMEM((3, PARTS, rows, width), jnp.bfloat16),
            pltpu.VMEM((3, PARTS, rows, width), jnp.bfloat16),
            pltpu.VMEM((n_cp, PARTS, rows, width), jnp.bfloat16),
            pltpu.VMEM((depth, wide), jnp.bfloat16),
            pltpu.VMEM((n_cp, rows, wide), jnp.float32),
            pltpu.VMEM((n_cp, half, wide), jnp.bfloat16),
            pltpu.VMEM((n_cp, half, wide), jnp.bfloat16),
            pltpu.VMEM((3, rows, n_cp * rows), jnp.float32),
            dma((2,)),
            dma,
            dma((PARTS,)),
            dma,
            dma((line, 2)),
            dma((line, 2)),
            dma((n_cp, 2)),
            dma,
            dma((2,)),
            dma((2, PARTS)),
            dma((3,)),
            dma((line,)),
            dma((line,)),
            dma((line,)),
            dma,
            dma,
            dma((n_cp, PARTS)),
            dma((n_cp,)),
            dma((n_cp,)),
        ],
        compiler_params=pltpu.CompilerParams(
            collective_id=0, has_side_effects=True, vmem_limit_bytes=50000 * 1024
        ),
    )(span_order, queries, keys, values, out_weight)


def solution(mesh):
    placed = (P("pp", "cp", "tp"), P("pp", "cp", "tp"), P("pp", "cp", "tp"), P("tp", "cp"), P())
    return jax.shard_map(
        functools.partial(on_device, mesh.shape["pp"], mesh.shape["cp"]),
        mesh=mesh,
        in_specs=placed,
        out_specs=P("pp", None, "tp", "cp"),
        check_vma=False,
    )
```
